32 devices in a mesh: blk: 8 (over z, x), grp: 4 (over y, core).
Axes of the slice: x: 2, y: 2, z: 4, core: 2. Of those that a mesh axis runs over, the one named last changes fastest.
Arguments:
- positions: float32 [3, 2048], P(None, ('blk', 'grp')), may hold values from -0.25 to 31.25, as said below
- moments: float32 [2, 2, 3, 2048], P(None, None, None, ('blk', 'grp')), may hold values from -6 to 6
- inv_polar_re: float32 [2048], P(('blk', 'grp')), may hold values from 0.5 to 2
- inv_polar_im: float32 [2048], P(('blk', 'grp')), may hold values from -0.5 to 0.5
- mode_field: float32 [2, 3, 2048, 512], P(None, None, ('blk', 'grp')), may hold values from -0.078125 to 0.078125
- mode_detune: float32 [512], replicated, may hold values from -1 to 1
- mode_width: float32 [512], replicated, may hold values from 0.05 to 1
Outputs:
- response: float32 [2, 2, 3, 2048], P(None, None, None, ('blk', 'grp'))
The draws below stay inside these ranges and needn't reach their ends.
Inputs may be any that keep to these rules, and one draw needn't show every extreme that they name: `positions`: dipole n lies within 0.25, in each coordinate, of the lattice site (n % 32, (n // 32) % 32, n // 1024); distinct dipoles are at least 0.5 apart.
All inputs are finite; a program needn't handle non-finite values.
Results may differ from the reference program's by a relative error of at most 0.0003.
Values sent between devices are 32-bit elements; how exact they have to be, the bound alone decides.
No kernel may reach another device: no remote copies, remote signals or barrier semaphores. Data moves between devices by JAX's collectives and lax.ppermute only.
A program may use at most 64 MiB of HBM per device.

```python
import math
import jax
import jax.numpy as jnp
from jax import lax

Q = 512
DRIVES = 2
NDIP = 2048


def draw_positions(key, part):
    ordinal = jnp.arange(NDIP, dtype=jnp.int32)
    column = (ordinal % 32).astype(jnp.float32)
    site_row = (ordinal // 32 % 32).astype(jnp.float32)
    depth_level = (ordinal // 1024).astype(jnp.float32)
    jitter_size = 0.2
    jitter = jax.random.uniform(key, (3, NDIP), jnp.float32, -jitter_size, jitter_size)
    return jnp.stack([column, site_row, depth_level]) + jitter


def shard_levels(rng, extent, split, least, largest):
    loudness, own = 1.0, jax.random.fold_in(rng, 6)
    for dim, shards_of in split:
        draws = jnp.exp(jax.random.uniform(jax.random.fold_in(own, dim), (shards_of,), jnp.float32, least / len(split), largest / len(split)))
        loudness = loudness * jnp.repeat(draws, extent[dim] // shards_of).reshape([-1 if axis == dim else 1 for axis in range(len(extent))])
    return loudness


def normal_values(rng, shape, deviation, reach, cuts=(), held_as=jnp.bfloat16):
    result = deviation * jax.random.normal(rng, shape, jnp.float32)
    if cuts:
        result = result * shard_levels(rng, shape, cuts, -0.22, 0.18)
    return jnp.clip(result, -reach, reach).astype(held_as)


def setup_inputs(seed: int = 0) -> dict:
    key_of = jax.random.split(jax.random.key(seed), 8)
    return {
        "positions": draw_positions(jax.random.fold_in(key_of[7], 71), 0),
        "moments": normal_values(key_of[1], (DRIVES, 2, 3, NDIP), 1.0, 6.0, ((3, 32),), jnp.float32),
        "inv_polar_re": jnp.clip(jnp.exp(math.log(2.0) - 1.3862944 * jax.random.uniform(key_of[2], (NDIP,), jnp.float32) ** shard_levels(key_of[2], (NDIP,), ((0, 32),), -0.2, 0.2)), 0.5, 2.0),
        "inv_polar_im": jnp.clip(jax.random.uniform(key_of[3], (NDIP,), jnp.float32, -0.5, 0.5) * shard_levels(key_of[3], (NDIP,), ((0, 32),), -0.4, 0.0), -0.5, 0.5),
        "mode_field": normal_values(key_of[4], (2, 3, NDIP, Q), (0.27 / (Q * 6 * NDIP) ** 0.25), 0.078125, ((2, 32),), jnp.float32),
        "mode_detune": jnp.clip(jax.random.uniform(key_of[5], (Q,), jnp.float32, -1.0, 1.0), -1.0, 1.0),
        "mode_width": jnp.clip(jnp.exp(jax.random.uniform(key_of[6], (Q,), jnp.float32, math.log(0.05), math.log(1.0))), 0.05, 1.0),
    }


wavenumber = 1.0
coupling = 0.05
near_limit = 0.04

def pair_field(deltas, dipoles, axis_sum):
    delta_x, delta_y, delta_z = deltas
    square = delta_x * delta_x + delta_y * delta_y + delta_z * delta_z
    coincide = square < near_limit
    safe_square = jnp.where(coincide, 1.0, square)
    inverse = 1.0 / jnp.sqrt(safe_square)
    phase_arg = wavenumber * safe_square * inverse
    cos_val = jnp.cos(phase_arg)
    sine_val = jnp.sin(phase_arg)
    masked_cube = jnp.where(coincide, 0.0, inverse * inverse * inverse)
    near_re = phase_arg * phase_arg - 1.0
    far_re = 3.0 - phase_arg * phase_arg
    diag_re = (cos_val * near_re - sine_val * phase_arg) * masked_cube
    diag_im = (sine_val * near_re + cos_val * phase_arg) * masked_cube
    scaled = masked_cube / safe_square
    outer_re = (cos_val * far_re + 3.0 * sine_val * phase_arg) * scaled
    outer_im = (sine_val * far_re - 3.0 * cos_val * phase_arg) * scaled
    tile_list = []
    for drive_set in range(len(dipoles) // 6):
        moment_re = dipoles[6 * drive_set:6 * drive_set + 3]
        moment_im = dipoles[6 * drive_set + 3:6 * drive_set + 6]
        proj_re = delta_x * moment_re[0] + delta_y * moment_re[1] + delta_z * moment_re[2]
        proj_im = delta_x * moment_im[0] + delta_y * moment_im[1] + delta_z * moment_im[2]
        along_re = outer_re * proj_re - outer_im * proj_im
        along_im = outer_re * proj_im + outer_im * proj_re
        for component in range(3):
            tile_list.append(diag_re * moment_re[component] - diag_im * moment_im[component] + deltas[component] * along_re)
        for component in range(3):
            tile_list.append(diag_re * moment_im[component] + diag_im * moment_re[component] + deltas[component] * along_im)
    return jnp.stack([lax.optimization_barrier(jnp.sum(entry_tile, axis=axis_sum)) for entry_tile in tile_list])

def contract(left, right):
    return lax.dot_general(left, right, (((0,), (1,)), ((), ())), precision=lax.Precision.HIGHEST)

def modal_project(mode_rows, moment_rows):
    amp_re = contract(mode_rows[0], moment_rows[:, 0]) - contract(mode_rows[1], moment_rows[:, 1])
    amp_im = contract(mode_rows[0], moment_rows[:, 1]) + contract(mode_rows[1], moment_rows[:, 0])
    return (amp_re, amp_im)

def spread(weights, rows):
    return lax.dot_general(weights, rows, (((0,), (1,)), ((), ())), precision=lax.Precision.HIGHEST)

def modal_spread(mode_rows, amp_re, amp_im, mode_detune, mode_width):
    denominator = mode_detune * mode_detune + mode_width * mode_width
    resp_re = (mode_detune / denominator)[:, None]
    resp_im = (mode_width / denominator)[:, None]
    weighted_re = resp_re * amp_re - resp_im * amp_im
    weighted_im = resp_re * amp_im + resp_im * amp_re
    out_re = spread(weighted_re, mode_rows[0]) - spread(weighted_im, mode_rows[1])
    out_im = spread(weighted_re, mode_rows[1]) + spread(weighted_im, mode_rows[0])
    return jnp.stack([out_re, out_im], axis=1)

def combine(moments, inv_polar_re, inv_polar_im, pair_part, modal_part):
    drives = moments.shape[0]
    dipole_count = moments.shape[3]
    field_sum = coupling * pair_part.reshape(drives, 2, 3, dipole_count) + modal_part.reshape(drives, 2, 3, dipole_count)
    moment_re = moments[:, 0]
    moment_im = moments[:, 1]
    resp_re = inv_polar_re * moment_re - inv_polar_im * moment_im - field_sum[:, 0]
    resp_im = inv_polar_re * moment_im + inv_polar_im * moment_re - field_sum[:, 1]
    return jnp.stack([resp_re, resp_im], axis=1)

def reference(positions, moments, inv_polar_re, inv_polar_im, mode_field, mode_detune, mode_width):
    drives = moments.shape[0]
    dipole_count = positions.shape[1]
    flat_moments = moments.reshape(drives * 6, dipole_count)
    source_mom = [flat_moments[member][None, :] for member in range(drives * 6)]
    block_rows = math.gcd(dipole_count, 128)

    def one_block(offset):
        target_pos = lax.dynamic_slice_in_dim(positions, offset, block_rows, 1)
        deltas = [target_pos[axis_c][:, None] - positions[axis_c][None, :] for axis_c in range(3)]
        return pair_field(deltas, source_mom, 1)
    starts = jnp.arange(dipole_count // block_rows, dtype=jnp.int32) * block_rows
    blocks = lax.map(one_block, starts)
    pair_part = jnp.transpose(blocks, (1, 0, 2)).reshape(drives * 6, dipole_count)
    mode_rows = mode_field.reshape(2, 3 * dipole_count, mode_field.shape[3])
    amp_re, amp_im = modal_project(mode_rows, moments.reshape(drives, 2, 3 * dipole_count))
    modal_part = modal_spread(mode_rows, amp_re, amp_im, mode_detune, mode_width).reshape(drives * 6, dipole_count)
    return combine(moments, inv_polar_re, inv_polar_im, pair_part, modal_part)
```

```python
import functools
import math

import jax
import jax.numpy as jnp
from jax import lax
from jax.experimental import pallas as pl
from jax.experimental.pallas import tpu as pltpu
from jax.sharding import PartitionSpec as P

wavenumber = 1.0
coupling = 0.05
near_limit = 0.04

AXES = ("blk", "grp")
LANES = 128
ROWS = 16
CHUNK = 2 * LANES

PI_HIGH = 3.140625
PI_LOW = math.pi - PI_HIGH
SIN_POLY = (-0.16666656732559204, 0.008332998491823673, -0.00019805235206149518, 2.5970118713303236e-06)
COS_POLY = (-0.4999992549419403, 0.04166382923722267, -0.0013854617718607187, 2.316308928129729e-05)


def horner(coefficients, value):
    total = jnp.full_like(value, coefficients[-1])
    for entry in coefficients[-2::-1]:
        total = total * value + entry
    return total


def green_terms(delta_x, delta_y, delta_z):
    square = delta_x * delta_x + delta_y * delta_y + delta_z * delta_z
    coincide = square < near_limit
    square = jnp.where(coincide, 1.0, square)
    inverse = lax.rsqrt(square)
    radius = square * inverse
    half_turns = jnp.floor(radius * (1.0 / math.pi) + 0.5)
    angle = (radius - half_turns * PI_HIGH) - half_turns * PI_LOW
    angle_sq = angle * angle
    sine = angle + angle * (angle_sq * horner(SIN_POLY, angle_sq))
    cosine = 1.0 + angle_sq * horner(COS_POLY, angle_sq)
    odd = (half_turns.astype(jnp.int32) & 1) == 1
    inverse_sq = inverse * inverse
    cube = inverse_sq * inverse
    cube = jnp.where(odd, -cube, cube)
    cube = jnp.where(coincide, 0.0, cube)
    fifth = cube * inverse_sq
    near = square - 1.0
    far = 3.0 - square
    sine_r = sine * radius
    cosine_r = cosine * radius
    return (
        (cosine * near - sine_r) * cube,
        (sine * near + cosine_r) * cube,
        (cosine * far + 3.0 * sine_r) * fifth,
        (sine * far - 3.0 * cosine_r) * fifth,
    )


def split(value):
    high = value.astype(jnp.bfloat16)
    return high, (value - high.astype(jnp.float32)).astype(jnp.bfloat16)


def dot_t(left, right):
    return lax.dot_general(left, right, (((1,), (1,)), ((), ())), preferred_element_type=jnp.float32)


def project_kernel(left_ref, mode_ref, amp_ref, high_ref, low_ref):
    mode_high, mode_low = split(mode_ref[...])
    high_ref[...] = mode_high
    low_ref[...] = mode_low
    left_high, left_low = split(left_ref[...])
    both = jnp.dot(jnp.concatenate([left_high, left_low], axis=0), mode_high, preferred_element_type=jnp.float32)
    amp = both[0:4] + both[4:8] + jnp.dot(left_high, mode_low, preferred_element_type=jnp.float32)
    for tile in range(amp.shape[1] // LANES):
        amp_ref[4 * tile : 4 * tile + 4, :] = amp[:, tile * LANES : (tile + 1) * LANES]


def pair_kernel(chips, centre_ref, target_ref, source_ref, out_ref, green_ref):
    targets = target_ref.shape[1]
    out_ref[...] = jnp.zeros_like(out_ref)
    centre = [centre_ref[axis_c] for axis_c in range(3)]

    def chunk(step):
        base = step * (2 * ROWS)
        if not isinstance(base, int):
            base = pl.multiple_of(base, 2 * ROWS)
        block = jnp.concatenate(
            [source_ref[pl.ds(base, ROWS), :], source_ref[pl.ds(base + ROWS, ROWS), :]], axis=1
        )
        place = [block[12 + axis_c : 13 + axis_c, :] for axis_c in range(3)]
        for group in range(targets // 8):
            for half in range(CHUNK // LANES):
                lanes = slice(half * LANES, (half + 1) * LANES)
                rows = slice(group * 8, group * 8 + 8)
                deltas = [
                    target_ref[axis_c, rows, :] - jnp.broadcast_to(place[axis_c][:, lanes], (8, LANES))
                    for axis_c in range(3)
                ]
                for part, tile in enumerate(green_terms(*deltas)):
                    green_ref[part * targets + group * 8 : part * targets + group * 8 + 8, lanes] = tile
        local = [place[axis_c] - centre[axis_c] for axis_c in range(3)]
        moment = [block[4 * axis_c : 4 * axis_c + 4, :] for axis_c in range(3)]
        along = moment[0] * local[0] + moment[1] * local[1] + moment[2] * local[2]
        features = jnp.concatenate(
            [block]
            + [block * local[axis_c] for axis_c in range(3)]
            + [along * local[axis_c] for axis_c in range(3)]
            + [jnp.zeros_like(along)],
            axis=0,
        )
        out_ref[...] += lax.dot_general(
            features,
            green_ref[...],
            (((1,), (1,)), ((), ())),
            precision=lax.Precision.HIGHEST,
            preferred_element_type=jnp.float32,
        )

    steps = chips // 2
    if steps <= 4:
        for step in range(steps):
            chunk(step)
    else:
        pl.loop(0, steps)(chunk)


def finish_kernel(
    amp_ref, high_ref, low_ref, detune_ref, width_ref, first_ref, second_ref, centre_ref, place_ref, moment_ref,
    polar_re_ref, polar_im_ref, out_ref,
):
    targets = place_ref.shape[1]
    tiles = detune_ref.shape[1] // LANES
    amp = jnp.concatenate([amp_ref[4 * tile : 4 * tile + 4, :] for tile in range(tiles)], axis=1)
    detune, width = detune_ref[...], width_ref[...]
    denominator = detune * detune + width * width
    resp_re, resp_im = detune / denominator, width / denominator
    weighted = []
    for drive in range(2):
        amp_re, amp_im = amp[2 * drive : 2 * drive + 1], amp[2 * drive + 1 : 2 * drive + 2]
        weighted += [resp_re * amp_re - resp_im * amp_im, resp_re * amp_im + resp_im * amp_re]
    weight_high, weight_low = split(jnp.concatenate(weighted, axis=0))
    both = dot_t(jnp.concatenate([weight_high, weight_low], axis=0), high_ref[...])
    modal = both[0:4] + both[4:8] + dot_t(weight_high, low_ref[...])

    raw = first_ref[...] + second_ref[...]
    near_re, near_im, far_re, far_im = [raw[:, part * targets : (part + 1) * targets] for part in range(4)]
    local = [place_ref[axis_c : axis_c + 1, :] - centre_ref[axis_c] for axis_c in range(3)]

    def rows_of(table, group, axis_c):
        start = group * ROWS + 4 * axis_c
        return table[start : start + 4]

    def combine_parts(real, imag):
        out = []
        for drive in range(2):
            out.append(real[2 * drive : 2 * drive + 1] - imag[2 * drive + 1 : 2 * drive + 2])
            out.append(real[2 * drive + 1 : 2 * drive + 2] + imag[2 * drive : 2 * drive + 1])
        return jnp.concatenate(out, axis=0)

    def outer(table, axis_c):
        straight = sum(local[j] * rows_of(table, 0, j) for j in range(3))
        dotted = sum(rows_of(table, 1 + j, j) for j in range(3))
        crossed = sum(local[j] * rows_of(table, 1 + axis_c, j) for j in range(3))
        return local[axis_c] * (straight - dotted) - crossed + rows_of(table, 4, axis_c)

    half = 3 * targets
    for axis_c in range(3):
        real = rows_of(near_re, 0, axis_c) + outer(far_re, axis_c)
        imag = rows_of(near_im, 0, axis_c) + outer(far_im, axis_c)
        pair = combine_parts(real, imag)
        mode_re = modal[:, axis_c * targets : (axis_c + 1) * targets]
        mode_im = modal[:, half + axis_c * targets : half + (axis_c + 1) * targets]
        field = coupling * pair + combine_parts(mode_re, mode_im)
        polar_re, polar_im = polar_re_ref[...], polar_im_ref[...]
        for drive in range(2):
            moment_re = moment_ref[drive, axis_c, 0:1, :]
            moment_im = moment_ref[drive, axis_c, 1:2, :]
            out_ref[drive, axis_c, 0:1, :] = (
                polar_re * moment_re - polar_im * moment_im - field[2 * drive : 2 * drive + 1]
            )
            out_ref[drive, axis_c, 1:2, :] = (
                polar_re * moment_im + polar_im * moment_re - field[2 * drive + 1 : 2 * drive + 2]
            )


def in_vmem(count):
    return [pl.BlockSpec(memory_space=pltpu.VMEM)] * count


def in_smem():
    return pl.BlockSpec(memory_space=pltpu.SMEM)


def on_device(devices, positions, moments, inv_polar_re, inv_polar_im, mode_field, mode_detune, mode_width):
    targets = positions.shape[1]
    modes = mode_field.shape[3]
    shape = jax.ShapeDtypeStruct

    def exchange(value, distance):
        return lax.ppermute(value, AXES, [(i, i ^ distance) for i in range(devices)])

    ordered = jnp.transpose(moments, (2, 0, 1, 3)).reshape(12, targets)
    own = jnp.concatenate([ordered, positions, jnp.zeros((1, targets), jnp.float32)], axis=0)
    other = exchange(own, 1)

    flat = moments.reshape(2, 2, 3 * targets)
    swapped = jnp.stack([-flat[:, 1], flat[:, 0]], axis=1)
    left = jnp.concatenate([flat, swapped], axis=2).reshape(4, 6 * targets)
    amp, mode_high, mode_low = pl.pallas_call(
        project_kernel,
        out_shape=(
            shape((4 * modes // LANES, LANES), jnp.float32),
            shape((6 * targets, modes), jnp.bfloat16),
            shape((6 * targets, modes), jnp.bfloat16),
        ),
        in_specs=in_vmem(2),
        out_specs=tuple(in_vmem(3)),
        cost_estimate=pl.CostEstimate(flops=2_000_000, bytes_accessed=1_600_000, transcendentals=0),
        name="project",
    )(left, mode_field.reshape(6 * targets, modes))

    centre = jnp.mean(positions, axis=1)
    target_cols = jnp.broadcast_to(positions[:, :, None], (3, targets, LANES))

    def pair(sources, chips):
        return pl.pallas_call(
            functools.partial(pair_kernel, chips),
            out_shape=shape((5 * ROWS, 4 * targets), jnp.float32),
            in_specs=[in_smem()] + in_vmem(2),
            out_specs=in_vmem(1)[0],
            scratch_shapes=[pltpu.VMEM((4 * targets, CHUNK), jnp.float32)],
            cost_estimate=pl.CostEstimate(
                flops=2 * 5 * ROWS * 4 * targets * chips * LANES, bytes_accessed=400_000, transcendentals=0
            ),
            name="pair",
        )(centre, target_cols, sources)

    gathered = jnp.concatenate([own, other], axis=1)
    distance = devices // 2
    first = None
    while distance > 1:
        chips = gathered.shape[0] // ROWS
        arrived = exchange(jnp.concatenate([gathered, amp], axis=0), distance)
        last = distance == 2
        if last:
            first = pair(gathered, chips)
        amp = amp + arrived[chips * ROWS :]
        if last:
            second = pair(arrived, chips)
        else:
            gathered = jnp.concatenate([gathered, arrived[: chips * ROWS]], axis=0)
        distance //= 2
    amp = amp + exchange(amp, 1)

    out = pl.pallas_call(
        finish_kernel,
        out_shape=shape((2, 3, 2, targets), jnp.float32),
        in_specs=in_vmem(7) + [in_smem()] + in_vmem(4),
        out_specs=in_vmem(1)[0],
        cost_estimate=pl.CostEstimate(flops=2_000_000, bytes_accessed=1_000_000, transcendentals=0),
        name="finish",
    )(
        amp,
        mode_high,
        mode_low,
        mode_detune[None],
        mode_width[None],
        first,
        second,
        centre,
        positions,
        jnp.transpose(moments, (0, 2, 1, 3)),
        inv_polar_re[None],
        inv_polar_im[None],
    )
    return jnp.transpose(out, (0, 2, 1, 3))


def solution(mesh):
    placed = (
        P(None, AXES),
        P(None, None, None, AXES),
        P(AXES),
        P(AXES),
        P(None, None, AXES, None),
        P(),
        P(),
    )
    return jax.shard_map(
        functools.partial(on_device, mesh.size),
        mesh=mesh,
        in_specs=placed,
        out_specs=P(None, None, None, AXES),
        check_vma=False,
    )
```

```python
import functools
import math

import jax
import jax.numpy as jnp
from jax import lax
from jax.experimental import pallas as pl
from jax.experimental.pallas import tpu as pltpu
from jax.sharding import PartitionSpec as P


coupling = 0.05
near_limit = 0.04

AXES = ("blk", "grp")
LANES = 128
ROWS = 16
CHUNK_TILES = 4
AMP_ROWS = 16
FEATURES = 64

PI_HIGH = 3.140625
PI_LOW = math.pi - PI_HIGH
SIN_POLY = (-0.16666656732559204, 0.008332998491823673, -0.00019805235206149518, 2.5970118713303236e-06)
COS_POLY = (-0.4999992549419403, 0.04166382923722267, -0.0013854617718607187, 2.316308928129729e-05)


def horner(coefficients, value):
    total = value * coefficients[-1] + coefficients[-2]
    for entry in coefficients[-3::-1]:
        total = total * value + entry
    return total


def green_terms(delta_x, delta_y, delta_z):
    square = delta_x * delta_x + delta_y * delta_y + delta_z * delta_z
    inverse = jnp.where(square < near_limit, 0.0, lax.rsqrt(square))
    radius = square * inverse
    turns = jnp.floor(radius * (0.5 / math.pi) + 0.5)
    angle = (radius * 0.5 - turns * PI_HIGH) - turns * PI_LOW
    angle_sq = angle * angle
    half_sine = angle + angle * (angle_sq * horner(SIN_POLY, angle_sq))
    half_cosine = 1.0 + angle_sq * horner(COS_POLY, angle_sq)
    twice = half_sine + half_sine
    inverse_sq = inverse * inverse
    cube = inverse_sq * inverse
    cosine = (1.0 - twice * half_sine) * cube
    sine = (twice * half_cosine) * cube
    near = square - 1.0
    sine_r = sine * radius
    cosine_r = cosine * radius
    near_re = cosine * near - sine_r
    near_im = sine * near + cosine_r
    mixed_re = cosine + sine_r
    mixed_im = sine - cosine_r
    return (
        near_re,
        near_im,
        (mixed_re + mixed_re - near_re) * inverse_sq,
        (mixed_im + mixed_im - near_im) * inverse_sq,
    )


def split(value):
    high = value.astype(jnp.bfloat16)
    return high, (value - high.astype(jnp.float32)).astype(jnp.bfloat16)


def dot_t(left, right):
    return lax.dot_general(left, right, (((1,), (1,)), ((), ())), preferred_element_type=jnp.float32)


def project_kernel(
    mode_hbm, moment_hbm, place_hbm, detune_hbm, width_hbm, polar_re_hbm, polar_im_hbm,
    amp_ref, mode_ref, moment_ref, place_ref, detune_ref, width_ref, polar_re_ref, polar_im_ref, mode_sem, sem,
):
    pieces = 2
    depth = mode_ref.shape[0] // pieces
    loads = [
        pltpu.make_async_copy(mode_hbm.at[pl.ds(i * depth, depth)], mode_ref.at[pl.ds(i * depth, depth)], mode_sem.at[i])
        for i in range(pieces)
    ]
    small = [
        pltpu.make_async_copy(source, target, sem.at[i])
        for i, (source, target) in enumerate(
            (
                (moment_hbm, moment_ref),
                (place_hbm, place_ref),
                (detune_hbm, detune_ref),
                (width_hbm, width_ref),
                (polar_re_hbm, polar_re_ref),
                (polar_im_hbm, polar_im_ref),
            )
        )
    ]
    small[0].start()
    for load in loads:
        load.start()
    for load in small[1:]:
        load.start()
    small[0].wait()
    plain, swapped = [], []
    for axis_c in range(3):
        plain.append(jnp.concatenate([moment_ref[0, axis_c], moment_ref[1, axis_c]], axis=0))
        swapped.append(
            jnp.concatenate(
                [
                    piece
                    for drive in range(2)
                    for piece in (-moment_ref[drive, axis_c, 1:2, :], moment_ref[drive, axis_c, 0:1, :])
                ],
                axis=0,
            )
        )
    left_high, left_low = split(jnp.concatenate(plain + swapped, axis=1))
    for load in loads:
        load.wait()
    mode_high, mode_low = split(mode_ref[...])
    both = jnp.dot(jnp.concatenate([left_high, left_low], axis=0), mode_high, preferred_element_type=jnp.float32)
    amp = both[0:4] + both[4:8] + jnp.dot(left_high, mode_low, preferred_element_type=jnp.float32)
    for tile in range(amp.shape[1] // LANES):
        amp_ref[4 * tile : 4 * tile + 4, :] = amp[:, tile * LANES : (tile + 1) * LANES]
    for load in small[1:]:
        load.wait()


def join_kernel(moment_ref, moment_other_ref, place_ref, place_other_ref, amp_ref, out_ref):
    for axis_c in range(3):
        for drive in range(2):
            row = 4 * axis_c + 2 * drive
            out_ref[row : row + 2, :] = jnp.concatenate(
                [moment_ref[drive, axis_c], moment_other_ref[drive, axis_c]], axis=1
            )
    out_ref[12:15, :] = jnp.concatenate([place_ref[...], place_other_ref[...]], axis=1)
    out_ref[15:16, :] = jnp.zeros((1, out_ref.shape[1]), jnp.float32)
    out_ref[ROWS:, :] = amp_ref[...]


def merge_kernel(*refs):
    out_ref = refs[-1]
    rows = refs[0].shape[0] - AMP_ROWS
    for place, ref in enumerate(refs[:-1]):
        out_ref[place * rows : (place + 1) * rows, :] = ref[:rows, :]
    out_ref[(len(refs) - 1) * rows :, :] = sum(ref[rows:, :] for ref in refs[:-1])


def total_kernel(*refs):
    start = refs[0].shape[0] - AMP_ROWS
    refs[-1][...] = sum(ref[start:, :] for ref in refs[:-1])


def prepare_kernel(
    mode_ref, place_ref, moment_ref, detune_ref, width_ref, polar_re_ref, polar_im_ref,
    high_ref, low_ref, column_ref, centre_ref, straight_ref, crossed_ref, base_ref,
):
    high_ref[...], low_ref[...] = split(jnp.transpose(mode_ref[...], (1, 0)))
    targets = place_ref.shape[1]
    for axis_c in range(3):
        row = place_ref[axis_c : axis_c + 1, :]
        column_ref[axis_c] = jnp.transpose(jnp.broadcast_to(row, (LANES, targets)), (1, 0))
        middle = jnp.sum(row, axis=1, keepdims=True) * (1.0 / targets)
        centre_ref[axis_c : axis_c + 1, :] = jnp.broadcast_to(middle, (1, LANES))
    detune, width = detune_ref[...], width_ref[...]
    denominator = detune * detune + width * width
    resp_re, resp_im = detune / denominator, width / denominator
    for tile in range(detune.shape[1] // LANES):
        lanes = slice(tile * LANES, (tile + 1) * LANES)
        for drive in range(2):
            row = 4 * tile + 2 * drive
            straight_ref[row : row + 2, :] = jnp.broadcast_to(resp_re[:, lanes], (2, LANES))
            crossed_ref[row : row + 1, :] = -resp_im[:, lanes]
            crossed_ref[row + 1 : row + 2, :] = resp_im[:, lanes]
    polar_re, polar_im = polar_re_ref[...], polar_im_ref[...]
    for axis_c in range(3):
        for drive in range(2):
            row = 4 * axis_c + 2 * drive
            moment_re = moment_ref[drive, axis_c, 0:1, :]
            moment_im = moment_ref[drive, axis_c, 1:2, :]
            base_ref[row : row + 1, :] = polar_re * moment_re - polar_im * moment_im
            base_ref[row + 1 : row + 2, :] = polar_re * moment_im + polar_im * moment_re


def accumulate_pairs(chips, centre_ref, target_ref, source_ref, out_ref, green_ref, feature_ref):
    targets = target_ref.shape[1]
    centre = [centre_ref[axis_c : axis_c + 1, 0:1] for axis_c in range(3)]

    def chunk(step, first):
        for tile in range(first, first + CHUNK_TILES):
            base = (step * CHUNK_TILES + tile - first) * ROWS
            if not isinstance(base, int):
                base = pl.multiple_of(base, ROWS)
            block = source_ref[pl.ds(base, ROWS), :]
            place = [block[12 + axis_c : 13 + axis_c, :] for axis_c in range(3)]
            local = [place[axis_c] - centre[axis_c] for axis_c in range(3)]
            moment = [block[4 * axis_c : 4 * axis_c + 4, :] for axis_c in range(3)]
            along = moment[0] * local[0] + moment[1] * local[1] + moment[2] * local[2]
            features = jnp.concatenate(
                [block[:12]]
                + [block[:12] * local[axis_c] for axis_c in range(3)]
                + [along * local[axis_c] for axis_c in range(3)]
                + [jnp.zeros_like(along)],
                axis=0,
            )
            high, (middle, low) = split3(features)
            feature_ref[tile, 0:FEATURES, :] = high
            feature_ref[tile, FEATURES : 2 * FEATURES, :] = middle
            feature_ref[tile, 2 * FEATURES :, :] = low
            for group in range(targets // 16):
                rows = slice(group * 16, group * 16 + 16)
                deltas = [
                    target_ref[axis_c, rows, :] - jnp.broadcast_to(place[axis_c], (16, LANES)) for axis_c in range(3)
                ]
                for part, entry in enumerate(green_terms(*deltas)):
                    start = part * targets + group * 16
                    high, rest = split3(entry, part >= 2)
                    green_ref[tile, start : start + 16, :] = high
                    green_ref[tile, 4 * targets + start : 4 * targets + start + 16, :] = rest[0]
                    if part >= 2:
                        green_ref[tile, 6 * targets + start : 6 * targets + start + 16, :] = rest[1]
        out_ref[...] += dot_t(
            jnp.concatenate([green_ref[tile] for tile in range(first, first + CHUNK_TILES)], axis=1),
            jnp.concatenate([feature_ref[tile] for tile in range(first, first + CHUNK_TILES)], axis=1),
        )

    steps = chips // CHUNK_TILES
    if steps == 1:
        chunk(0, 0)
    else:
        pl.loop(0, steps)(lambda step: chunk(step, 0))


def split3(value, three=True):
    high = value.astype(jnp.bfloat16)
    rest = value - high.astype(jnp.float32)
    middle = rest.astype(jnp.bfloat16)
    if not three:
        return high, (middle,)
    return high, (middle, (rest - middle.astype(jnp.float32)).astype(jnp.bfloat16))


def first_pair_kernel(chips, centre_ref, target_ref, source_ref, out_ref, green_ref, feature_ref):
    out_ref[...] = jnp.zeros_like(out_ref)
    accumulate_pairs(chips, centre_ref, target_ref, source_ref, out_ref, green_ref, feature_ref)


def next_pair_kernel(chips, centre_ref, target_ref, source_ref, before_ref, out_ref, green_ref, feature_ref):
    out_ref[...] = before_ref[...]
    accumulate_pairs(chips, centre_ref, target_ref, source_ref, out_ref, green_ref, feature_ref)


def complex_rows(real, imag):
    out = []
    for drive in range(2):
        out.append(real[2 * drive : 2 * drive + 1] - imag[2 * drive + 1 : 2 * drive + 2])
        out.append(real[2 * drive + 1 : 2 * drive + 2] + imag[2 * drive : 2 * drive + 1])
    return jnp.concatenate(out, axis=0)


def last_pair_kernel(
    chips, centre_ref, target_ref, source_ref, first_ref, place_ref, base_ref, out_ref, sum_ref, green_ref, feature_ref
):
    sum_ref[...] = first_ref[...]
    accumulate_pairs(chips, centre_ref, target_ref, source_ref, sum_ref, green_ref, feature_ref)
    targets = place_ref.shape[1]
    raw = sum_ref[0 : 4 * targets, :] + sum_ref[4 * targets : 8 * targets, :]
    raw = jnp.concatenate([raw[: 2 * targets], raw[2 * targets :] + sum_ref[8 * targets :, :]], axis=0)
    raw = jnp.transpose(raw, (1, 0))
    raw = raw[0:FEATURES] + raw[FEATURES : 2 * FEATURES] + raw[2 * FEATURES :]
    near_re, near_im, far_re, far_im = [raw[:, part * targets : (part + 1) * targets] for part in range(4)]
    local = [place_ref[axis_c : axis_c + 1, :] - centre_ref[axis_c : axis_c + 1, 0:1] for axis_c in range(3)]

    def rows_of(table, group, axis_c):
        return table[12 * group + 4 * axis_c : 12 * group + 4 * axis_c + 4]

    def outer(table, axis_c):
        straight = sum(local[j] * rows_of(table, 0, j) for j in range(3))
        dotted = sum(rows_of(table, 1 + j, j) for j in range(3))
        crossed = sum(local[j] * rows_of(table, 1 + axis_c, j) for j in range(3))
        return local[axis_c] * (straight - dotted) - crossed + rows_of(table, 4, axis_c)

    for axis_c in range(3):
        pair = complex_rows(
            rows_of(near_re, 0, axis_c) + outer(far_re, axis_c), rows_of(near_im, 0, axis_c) + outer(far_im, axis_c)
        )
        out_ref[4 * axis_c : 4 * axis_c + 4, :] = base_ref[4 * axis_c : 4 * axis_c + 4, :] - coupling * pair


def finish_kernel(mine_ref, other_ref, high_ref, low_ref, straight_ref, crossed_ref, rest_ref, out_ref):
    targets = rest_ref.shape[1]
    amp = mine_ref[...] + other_ref[...]
    rows = amp.shape[0]
    odd = (lax.broadcasted_iota(jnp.int32, amp.shape, 0) & 1) == 1
    partner = jnp.where(odd, pltpu.roll(amp, 1, 0), pltpu.roll(amp, rows - 1, 0))
    weighted = straight_ref[...] * amp + crossed_ref[...] * partner
    weighted = jnp.concatenate([weighted[4 * tile : 4 * tile + 4] for tile in range(rows // 4)], axis=1)
    weight_high, weight_low = split(weighted)
    both = jnp.dot(
        jnp.concatenate([weight_high, weight_low], axis=0), high_ref[...], preferred_element_type=jnp.float32
    )
    modal = both[0:4] + both[4:8] + jnp.dot(weight_high, low_ref[...], preferred_element_type=jnp.float32)
    half = 3 * targets
    for axis_c in range(3):
        mode_re = modal[:, axis_c * targets : (axis_c + 1) * targets]
        mode_im = modal[:, half + axis_c * targets : half + (axis_c + 1) * targets]
        result = rest_ref[4 * axis_c : 4 * axis_c + 4, :] - complex_rows(mode_re, mode_im)
        out_ref[0, axis_c] = result[0:2]
        out_ref[1, axis_c] = result[2:4]


def kernel_call(body, outs, operands, scratch=(), flops=100_000, loads=False):
    single = not isinstance(outs, tuple)
    vmem = pl.BlockSpec(memory_space=pltpu.VMEM)
    source = pl.BlockSpec(memory_space=pltpu.HBM) if loads else vmem
    return pl.pallas_call(
        body,
        out_shape=outs,
        in_specs=[source] * len(operands),
        out_specs=vmem if single else (vmem,) * len(outs),
        scratch_shapes=list(scratch),
        cost_estimate=pl.CostEstimate(flops=flops, bytes_accessed=100_000, transcendentals=0),
        compiler_params=pltpu.CompilerParams(vmem_limit_bytes=12 * 1024 * 1024),
    )(*operands)


def on_device(devices, positions, moments, inv_polar_re, inv_polar_im, mode_field, mode_detune, mode_width):
    targets = positions.shape[1]
    modes = mode_field.shape[3]

    def shape(*dims, dtype=jnp.float32):
        return jax.ShapeDtypeStruct(dims, dtype)

    def exchange(value, distance):
        return lax.ppermute(value, AXES, [(i, i ^ distance) for i in range(devices)])

    def like(value):
        return shape(*value.shape)

    moments = jnp.transpose(moments, (0, 2, 1, 3))
    mode_rows = mode_field.reshape(6 * targets, modes)
    moments_other = exchange(moments, 1)
    positions_other = exchange(positions, 1)
    inputs = tuple(pltpu.with_memory_space_constraint(value, pltpu.HBM) for value in (
        mode_rows,
        moments,
        positions,
        mode_detune[None],
        mode_width[None],
        inv_polar_re[None],
        inv_polar_im[None],
    ))
    amp, mode_rows, moments, positions, detune, width, polar_re, polar_im = kernel_call(
        project_kernel,
        (shape(AMP_ROWS, LANES),) + tuple(like(value) for value in inputs),
        inputs,
        [pltpu.SemaphoreType.DMA((2,)), pltpu.SemaphoreType.DMA((6,))],
        flops=5_000_000,
        loads=True,
    )
    message = kernel_call(
        join_kernel, shape(ROWS + AMP_ROWS, LANES), (moments, moments_other, positions, positions_other, amp)
    )
    mode_high, mode_low, columns, centre, straight, crossed, base = kernel_call(
        prepare_kernel,
        (
            shape(modes, 6 * targets, dtype=jnp.bfloat16),
            shape(modes, 6 * targets, dtype=jnp.bfloat16),
            shape(3, targets, LANES),
            shape(8, LANES),
            shape(AMP_ROWS, LANES),
            shape(AMP_ROWS, LANES),
            shape(12, targets),
        ),
        (mode_rows, positions, moments, detune, width, polar_re, polar_im),
        flops=5_000_000,
    )
    distance = devices // 2
    while distance > 4:
        steps = (distance ^ 1, (3 * distance // 2) ^ 1, distance // 2) if distance > 8 else (distance ^ 1,)
        arrived = [exchange(message, step) for step in steps]
        rows = message.shape[0] - AMP_ROWS
        message = kernel_call(merge_kernel, shape((1 + len(steps)) * rows + AMP_ROWS, LANES), (message, *arrived))
        distance //= 4 if len(steps) == 3 else 2
    chips = (message.shape[0] - AMP_ROWS) // ROWS
    diagonal = exchange(message, 6)
    side = exchange(message, 4 ^ 1)
    near = exchange(message, 2 ^ 1)
    sums = shape(10 * targets, 3 * FEATURES)
    scratch = [
        pltpu.VMEM((CHUNK_TILES, 10 * targets, LANES), jnp.bfloat16),
        pltpu.VMEM((CHUNK_TILES, 3 * FEATURES, LANES), jnp.bfloat16),
    ]

    def pair(kernel, source, *more, out=sums, extra=()):
        return kernel_call(
            functools.partial(kernel, chips),
            out,
            (centre, columns, source) + more,
            list(extra) + scratch,
            flops=20_000_000,
        )

    partial_sums = pair(first_pair_kernel, message)
    partial_sums = pair(next_pair_kernel, diagonal, partial_sums)
    mine = kernel_call(total_kernel, shape(AMP_ROWS, LANES), (message, diagonal, side, near))
    other = exchange(mine, 1)
    partial_sums = pair(next_pair_kernel, side, partial_sums)
    rest = pair(
        last_pair_kernel,
        near,
        partial_sums,
        positions,
        base,
        out=shape(12, targets),
        extra=(pltpu.VMEM(sums.shape, jnp.float32),),
    )
    out = kernel_call(
        finish_kernel, shape(2, 3, 2, targets), (mine, other, mode_high, mode_low, straight, crossed, rest)
    )
    return jnp.transpose(out, (0, 2, 1, 3))


def solution(mesh):
    placed = (
        P(None, AXES),
        P(None, None, None, AXES),
        P(AXES),
        P(AXES),
        P(None, None, AXES, None),
        P(),
        P(),
    )
    return jax.shard_map(
        functools.partial(on_device, mesh.size),
        mesh=mesh,
        in_specs=placed,
        out_specs=P(None, None, None, AXES),
        check_vma=False,
    )
```

```python
import functools
import math

import jax
import jax.numpy as jnp
from jax import lax
from jax.experimental import pallas as pl
from jax.experimental.pallas import tpu as pltpu
from jax.sharding import PartitionSpec as P


coupling = 0.05
near_limit = 0.04

AXES = ("blk", "grp")
LANES = 128
ROWS = 16
CHUNK_TILES = 4
PIECES = 3
AMP_ROWS = 16
FEATURES = 64
GROUP = 32

PI_HIGH = 3.140625
PI_LOW = math.pi - PI_HIGH
SIN_POLY = (-0.16666656732559204, 0.008332998491823673, -0.00019805235206149518, 2.5970118713303236e-06)
COS_POLY = (-0.4999992549419403, 0.04166382923722267, -0.0013854617718607187, 2.316308928129729e-05)


def horner(coefficients, value):
    total = value * coefficients[-1] + coefficients[-2]
    for entry in coefficients[-3::-1]:
        total = total * value + entry
    return total


def green_terms(delta_x, delta_y, delta_z):
    square = delta_x * delta_x + delta_y * delta_y + delta_z * delta_z
    inverse = jnp.where(square < near_limit, 0.0, lax.rsqrt(square))
    radius = square * inverse
    turns = jnp.floor(radius * (0.5 / math.pi) + 0.5)
    angle = (radius * 0.5 - turns * PI_HIGH) - turns * PI_LOW
    angle_sq = angle * angle
    half_sine = angle + angle * (angle_sq * horner(SIN_POLY, angle_sq))
    half_cosine = 1.0 + angle_sq * horner(COS_POLY, angle_sq)
    twice = half_sine + half_sine
    inverse_sq = inverse * inverse
    cube = inverse_sq * inverse
    cosine = (1.0 - twice * half_sine) * cube
    sine = (twice * half_cosine) * cube
    near = square - 1.0
    sine_r = sine * radius
    cosine_r = cosine * radius
    near_re = cosine * near - sine_r
    near_im = sine * near + cosine_r
    mixed_re = cosine + sine_r
    mixed_im = sine - cosine_r
    return (
        near_re,
        near_im,
        (mixed_re + mixed_re - near_re) * inverse_sq,
        (mixed_im + mixed_im - near_im) * inverse_sq,
    )


def split(value):
    high = value.astype(jnp.bfloat16)
    return high, (value - high.astype(jnp.float32)).astype(jnp.bfloat16)


def dot_t(left, right):
    return lax.dot_general(left, right, (((1,), (1,)), ((), ())), preferred_element_type=jnp.float32)


def project_kernel(mode_hbm, moment_hbm, place_hbm, amp_ref, mode_ref, moment_ref, place_ref, mode_sem, sem):
    pieces = PIECES
    depth = mode_ref.shape[0] // pieces
    loads = [
        pltpu.make_async_copy(mode_hbm.at[pl.ds(i * depth, depth)], mode_ref.at[pl.ds(i * depth, depth)], mode_sem.at[i])
        for i in range(pieces)
    ]
    small = [
        pltpu.make_async_copy(moment_hbm, moment_ref, sem.at[0]),
        pltpu.make_async_copy(place_hbm, place_ref, sem.at[1]),
    ]
    small[0].start()
    for load in loads:
        load.start()
    for load in small[1:]:
        load.start()
    small[0].wait()
    plain, swapped = [], []
    for axis_c in range(3):
        plain.append(jnp.concatenate([moment_ref[0, axis_c], moment_ref[1, axis_c]], axis=0))
        swapped.append(
            jnp.concatenate(
                [
                    piece
                    for drive in range(2)
                    for piece in (-moment_ref[drive, axis_c, 1:2, :], moment_ref[drive, axis_c, 0:1, :])
                ],
                axis=0,
            )
        )
    left_high, left_low = split(jnp.concatenate(plain + swapped, axis=1))
    both_left = jnp.concatenate([left_high, left_low], axis=0)
    both, rest = 0.0, 0.0
    for i, load in enumerate(loads):
        load.wait()
        piece = slice(i * depth, (i + 1) * depth)
        mode_high, mode_low = split(mode_ref[piece, :])
        both += jnp.dot(both_left[:, piece], mode_high, preferred_element_type=jnp.float32)
        rest += jnp.dot(left_high[:, piece], mode_low, preferred_element_type=jnp.float32)
    amp = both[0:4] + both[4:8] + rest
    for tile in range(amp.shape[1] // LANES):
        amp_ref[4 * tile : 4 * tile + 4, :] = amp[:, tile * LANES : (tile + 1) * LANES]
    for load in small[1:]:
        load.wait()


def join_kernel(moment_ref, moment_other_ref, place_ref, place_other_ref, amp_ref, out_ref):
    for axis_c in range(3):
        for drive in range(2):
            row = 4 * axis_c + 2 * drive
            out_ref[row : row + 2, :] = jnp.concatenate(
                [moment_ref[drive, axis_c], moment_other_ref[drive, axis_c]], axis=1
            )
    out_ref[12:15, :] = jnp.concatenate([place_ref[...], place_other_ref[...]], axis=1)
    out_ref[15:16, :] = jnp.zeros((1, out_ref.shape[1]), jnp.float32)
    out_ref[ROWS:, :] = amp_ref[...]


def merge_kernel(*refs):
    out_ref = refs[-1]
    rows = refs[0].shape[0] - AMP_ROWS
    for place, ref in enumerate(refs[:-1]):
        out_ref[place * rows : (place + 1) * rows, :] = ref[:rows, :]
    out_ref[(len(refs) - 1) * rows :, :] = sum(ref[rows:, :] for ref in refs[:-1])


def total_kernel(*refs):
    start = refs[0].shape[0] - AMP_ROWS
    refs[-1][...] = sum(ref[start:, :] for ref in refs[:-1])


def prepare_kernel(
    mode_ref, place_ref, moment_ref, detune_hbm, width_hbm, polar_re_hbm, polar_im_hbm,
    high_ref, low_ref, column_ref, centre_ref, straight_ref, crossed_ref, base_ref,
    detune_ref, width_ref, polar_re_ref, polar_im_ref, sem,
):
    loads = [
        pltpu.make_async_copy(source, target, sem.at[i])
        for i, (source, target) in enumerate(
            (
                (detune_hbm, detune_ref),
                (width_hbm, width_ref),
                (polar_re_hbm, polar_re_ref),
                (polar_im_hbm, polar_im_ref),
            )
        )
    ]
    for load in loads:
        load.start()
    high_ref[...], low_ref[...] = split(jnp.transpose(mode_ref[...], (1, 0)))
    targets = place_ref.shape[1]
    for axis_c in range(3):
        row = place_ref[axis_c : axis_c + 1, :]
        column_ref[axis_c] = jnp.transpose(jnp.broadcast_to(row, (LANES, targets)), (1, 0))
        middle = jnp.sum(row, axis=1, keepdims=True) * (1.0 / targets)
        centre_ref[axis_c : axis_c + 1, :] = jnp.broadcast_to(middle, (1, LANES))
    for load in loads:
        load.wait()
    detune, width = detune_ref[...], width_ref[...]
    denominator = detune * detune + width * width
    resp_re, resp_im = detune / denominator, width / denominator
    for tile in range(detune.shape[1] // LANES):
        lanes = slice(tile * LANES, (tile + 1) * LANES)
        for drive in range(2):
            row = 4 * tile + 2 * drive
            straight_ref[row : row + 2, :] = jnp.broadcast_to(resp_re[:, lanes], (2, LANES))
            crossed_ref[row : row + 1, :] = -resp_im[:, lanes]
            crossed_ref[row + 1 : row + 2, :] = resp_im[:, lanes]
    polar_re, polar_im = polar_re_ref[...], polar_im_ref[...]
    for axis_c in range(3):
        for drive in range(2):
            row = 4 * axis_c + 2 * drive
            moment_re = moment_ref[drive, axis_c, 0:1, :]
            moment_im = moment_ref[drive, axis_c, 1:2, :]
            base_ref[row : row + 1, :] = polar_re * moment_re - polar_im * moment_im
            base_ref[row + 1 : row + 2, :] = polar_re * moment_im + polar_im * moment_re


def accumulate_pairs(chips, centre_ref, target_ref, source_refs, before_ref, out_ref, green_ref, feature_ref):
    groups = target_ref.shape[1] // GROUP
    depth = 10 * GROUP
    centre = [centre_ref[axis_c : axis_c + 1, 0:1] for axis_c in range(3)]

    tiles = CHUNK_TILES * len(source_refs)

    def chunk(step, before_ref):
        places = []
        for tile in range(tiles):
            base = (step * CHUNK_TILES + tile % CHUNK_TILES) * ROWS
            if not isinstance(base, int):
                base = pl.multiple_of(base, ROWS)
            block = source_refs[tile // CHUNK_TILES][pl.ds(base, ROWS), :]
            place = [block[12 + axis_c : 13 + axis_c, :] for axis_c in range(3)]
            places.append([jnp.broadcast_to(row, (16, LANES)) for row in place])
            local = [place[axis_c] - centre[axis_c] for axis_c in range(3)]
            moment = [block[4 * axis_c : 4 * axis_c + 4, :] for axis_c in range(3)]
            along = moment[0] * local[0] + moment[1] * local[1] + moment[2] * local[2]
            features = jnp.concatenate(
                [block[:12]]
                + [block[:12] * local[axis_c] for axis_c in range(3)]
                + [along * local[axis_c] for axis_c in range(3)]
                + [jnp.zeros_like(along)],
                axis=0,
            )
            high, (middle, low) = split3(features)
            feature_ref[tile, 0:FEATURES, :] = high
            feature_ref[tile, FEATURES : 2 * FEATURES, :] = middle
            feature_ref[tile, 2 * FEATURES :, :] = low
        for group in range(groups):
            for tile in range(tiles):
                for piece in range(GROUP // 16):
                    rows = slice(group * GROUP + piece * 16, group * GROUP + piece * 16 + 16)
                    deltas = [target_ref[axis_c, rows, :] - places[tile][axis_c] for axis_c in range(3)]
                    for part, entry in enumerate(green_terms(*deltas)):
                        high, rest = split3(entry, part >= 2)
                        for level, value in enumerate((high,) + rest):
                            start = group * depth + (level * 4 + part - (2 if level == 2 else 0)) * GROUP + piece * 16
                            green_ref[tile, start : start + 16, :] = value
            rows = slice(group * depth, (group + 1) * depth)
            sums = dot_t(
                jnp.concatenate([green_ref[tile, rows, :] for tile in range(tiles)], axis=1),
                jnp.concatenate([feature_ref[tile] for tile in range(tiles)], axis=1),
            )
            out_ref[rows, :] = sums if before_ref is None else before_ref[rows, :] + sums

    chunk(0, before_ref)
    if chips > CHUNK_TILES:
        pl.loop(1, chips // CHUNK_TILES)(lambda step: chunk(step, out_ref))


def split3(value, three=True):
    high = value.astype(jnp.bfloat16)
    rest = value - high.astype(jnp.float32)
    middle = rest.astype(jnp.bfloat16)
    if not three:
        return high, (middle,)
    return high, (middle, (rest - middle.astype(jnp.float32)).astype(jnp.bfloat16))


def first_pair_kernel(chips, centre_ref, target_ref, source_ref, out_ref, green_ref, feature_ref):
    accumulate_pairs(chips, centre_ref, target_ref, (source_ref,), None, out_ref, green_ref, feature_ref)


def next_pair_kernel(chips, centre_ref, target_ref, source_ref, before_ref, out_ref, green_ref, feature_ref):
    accumulate_pairs(chips, centre_ref, target_ref, (source_ref,), before_ref, out_ref, green_ref, feature_ref)


def complex_rows(real, imag):
    out = []
    for drive in range(2):
        out.append(real[2 * drive : 2 * drive + 1] - imag[2 * drive + 1 : 2 * drive + 2])
        out.append(real[2 * drive + 1 : 2 * drive + 2] + imag[2 * drive : 2 * drive + 1])
    return jnp.concatenate(out, axis=0)


def last_pair_kernel(
    chips, centre_ref, target_ref, side_ref, near_ref, first_ref, place_ref, base_ref, out_ref, sum_ref, green_ref,
    feature_ref,
):
    accumulate_pairs(chips, centre_ref, target_ref, (side_ref, near_ref), first_ref, sum_ref, green_ref, feature_ref)
    targets = place_ref.shape[1]

    def level(entry, part):
        starts = [group * 10 * GROUP + (entry * 4 + part) * GROUP for group in range(targets // GROUP)]
        return jnp.concatenate([sum_ref[start : start + GROUP, :] for start in starts], axis=0)

    raw = jnp.concatenate(
        [level(0, part) + level(1, part) + (level(2, part - 2) if part >= 2 else 0.0) for part in range(4)], axis=0
    )
    raw = jnp.transpose(raw, (1, 0))
    raw = raw[0:FEATURES] + raw[FEATURES : 2 * FEATURES] + raw[2 * FEATURES :]
    near_re, near_im, far_re, far_im = [raw[:, part * targets : (part + 1) * targets] for part in range(4)]
    local = [place_ref[axis_c : axis_c + 1, :] - centre_ref[axis_c : axis_c + 1, 0:1] for axis_c in range(3)]

    def rows_of(table, group, axis_c):
        return table[12 * group + 4 * axis_c : 12 * group + 4 * axis_c + 4]

    def outer(table, axis_c):
        straight = sum(local[j] * rows_of(table, 0, j) for j in range(3))
        dotted = sum(rows_of(table, 1 + j, j) for j in range(3))
        crossed = sum(local[j] * rows_of(table, 1 + axis_c, j) for j in range(3))
        return local[axis_c] * (straight - dotted) - crossed + rows_of(table, 4, axis_c)

    for axis_c in range(3):
        pair = complex_rows(
            rows_of(near_re, 0, axis_c) + outer(far_re, axis_c), rows_of(near_im, 0, axis_c) + outer(far_im, axis_c)
        )
        out_ref[4 * axis_c : 4 * axis_c + 4, :] = base_ref[4 * axis_c : 4 * axis_c + 4, :] - coupling * pair


def finish_kernel(mine_ref, other_ref, high_ref, low_ref, straight_ref, crossed_ref, rest_ref, out_ref):
    targets = rest_ref.shape[1]
    amp = mine_ref[...] + other_ref[...]
    rows = amp.shape[0]
    odd = (lax.broadcasted_iota(jnp.int32, amp.shape, 0) & 1) == 1
    partner = jnp.where(odd, pltpu.roll(amp, 1, 0), pltpu.roll(amp, rows - 1, 0))
    weighted = straight_ref[...] * amp + crossed_ref[...] * partner
    weighted = jnp.concatenate([weighted[4 * tile : 4 * tile + 4] for tile in range(rows // 4)], axis=1)
    weight_high, weight_low = split(weighted)
    both = jnp.dot(
        jnp.concatenate([weight_high, weight_low], axis=0), high_ref[...], preferred_element_type=jnp.float32
    )
    modal = both[0:4] + both[4:8] + jnp.dot(weight_high, low_ref[...], preferred_element_type=jnp.float32)
    half = 3 * targets
    for axis_c in range(3):
        mode_re = modal[:, axis_c * targets : (axis_c + 1) * targets]
        mode_im = modal[:, half + axis_c * targets : half + (axis_c + 1) * targets]
        result = rest_ref[4 * axis_c : 4 * axis_c + 4, :] - complex_rows(mode_re, mode_im)
        out_ref[0, axis_c] = result[0:2]
        out_ref[1, axis_c] = result[2:4]


def kernel_call(body, outs, operands, scratch=(), flops=100_000, loads=()):
    single = not isinstance(outs, tuple)
    vmem = pl.BlockSpec(memory_space=pltpu.VMEM)
    hbm = pl.BlockSpec(memory_space=pltpu.HBM)
    return pl.pallas_call(
        body,
        out_shape=outs,
        in_specs=[vmem] * len(operands) + [hbm] * len(loads),
        out_specs=vmem if single else (vmem,) * len(outs),
        scratch_shapes=list(scratch),
        cost_estimate=pl.CostEstimate(flops=flops, bytes_accessed=100_000, transcendentals=0),
        compiler_params=pltpu.CompilerParams(vmem_limit_bytes=12 * 1024 * 1024),
    )(*operands, *loads)


def on_device(devices, positions, moments, inv_polar_re, inv_polar_im, mode_field, mode_detune, mode_width):
    targets = positions.shape[1]
    modes = mode_field.shape[3]

    def shape(*dims, dtype=jnp.float32):
        return jax.ShapeDtypeStruct(dims, dtype)

    def exchange(value, distance):
        return lax.ppermute(value, AXES, [(i, i ^ distance) for i in range(devices)])

    def like(value):
        return shape(*value.shape)

    moments = jnp.transpose(moments, (0, 2, 1, 3))
    mode_rows = mode_field.reshape(6 * targets, modes)
    moments_other = exchange(moments, 1)
    positions_other = exchange(positions, 1)

    def in_hbm(*values):
        return tuple(pltpu.with_memory_space_constraint(value, pltpu.HBM) for value in values)

    inputs = in_hbm(mode_rows, moments, positions)
    amp, mode_rows, moments, positions = kernel_call(
        project_kernel,
        (shape(AMP_ROWS, LANES),) + tuple(like(value) for value in inputs),
        (),
        [pltpu.SemaphoreType.DMA((PIECES,)), pltpu.SemaphoreType.DMA((2,))],
        flops=5_000_000,
        loads=inputs,
    )
    message = kernel_call(
        join_kernel, shape(ROWS + AMP_ROWS, LANES), (moments, moments_other, positions, positions_other, amp)
    )
    mode_high, mode_low, columns, centre, straight, crossed, base = kernel_call(
        prepare_kernel,
        (
            shape(modes, 6 * targets, dtype=jnp.bfloat16),
            shape(modes, 6 * targets, dtype=jnp.bfloat16),
            shape(3, targets, LANES),
            shape(8, LANES),
            shape(AMP_ROWS, LANES),
            shape(AMP_ROWS, LANES),
            shape(12, targets),
        ),
        (mode_rows, positions, moments),
        [
            pltpu.VMEM((1, modes), jnp.float32),
            pltpu.VMEM((1, modes), jnp.float32),
            pltpu.VMEM((1, targets), jnp.float32),
            pltpu.VMEM((1, targets), jnp.float32),
            pltpu.SemaphoreType.DMA((4,)),
        ],
        flops=5_000_000,
        loads=in_hbm(mode_detune[None], mode_width[None], inv_polar_re[None], inv_polar_im[None]),
    )
    distance = devices // 2
    while distance > 4:
        steps = ((3 * distance // 2) ^ 1, distance ^ 1, distance // 2) if distance > 8 else (distance ^ 1,)
        arrived = [exchange(message, step) for step in steps]
        rows = message.shape[0] - AMP_ROWS
        message = kernel_call(merge_kernel, shape((1 + len(steps)) * rows + AMP_ROWS, LANES), (message, *arrived))
        distance //= 4 if len(steps) == 3 else 2
    chips = (message.shape[0] - AMP_ROWS) // ROWS
    diagonal = exchange(message, 6)
    side = exchange(message, 4 ^ 1)
    near = exchange(message, 2 ^ 1)
    sums = shape(10 * targets, 3 * FEATURES)

    def pair(kernel, sources, *more, out=sums, extra=()):
        tiles = CHUNK_TILES * len(sources)
        return kernel_call(
            functools.partial(kernel, chips),
            out,
            (centre, columns) + sources + more,
            list(extra)
            + [
                pltpu.VMEM((tiles, 10 * targets, LANES), jnp.bfloat16),
                pltpu.VMEM((tiles, 3 * FEATURES, LANES), jnp.bfloat16),
            ],
            flops=20_000_000,
        )

    partial_sums = pair(first_pair_kernel, (message,))
    partial_sums = pair(next_pair_kernel, (diagonal,), partial_sums)
    mine = kernel_call(total_kernel, shape(AMP_ROWS, LANES), (message, diagonal, side, near))
    other = exchange(mine, 1)
    rest = pair(
        last_pair_kernel,
        (side, near),
        partial_sums,
        positions,
        base,
        out=shape(12, targets),
        extra=(pltpu.VMEM(sums.shape, jnp.float32),),
    )
    out = kernel_call(
        finish_kernel, shape(2, 3, 2, targets), (mine, other, mode_high, mode_low, straight, crossed, rest)
    )
    return jnp.transpose(out, (0, 2, 1, 3))


def solution(mesh):
    placed = (
        P(None, AXES),
        P(None, None, None, AXES),
        P(AXES),
        P(AXES),
        P(None, None, AXES, None),
        P(),
        P(),
    )
    return jax.shard_map(
        functools.partial(on_device, mesh.size),
        mesh=mesh,
        in_specs=placed,
        out_specs=P(None, None, None, AXES),
        check_vma=False,
    )
```

```python
import functools
import math

import jax
import jax.numpy as jnp
from jax import lax
from jax.experimental import pallas as pl
from jax.experimental.pallas import tpu as pltpu
from jax.sharding import PartitionSpec as P


coupling = 0.05
near_limit = 0.04

AXES = ("blk", "grp")
LANES = 128
ROWS = 16
CHUNK_TILES = 4
PIECES = 3
AMP_ROWS = 16
FEATURES = 64

PI_HIGH = 3.140625
PI_LOW = math.pi - PI_HIGH
SIN_POLY = (-0.16666656732559204, 0.008332998491823673, -0.00019805235206149518, 2.5970118713303236e-06)
COS_POLY = (-0.4999992549419403, 0.04166382923722267, -0.0013854617718607187, 2.316308928129729e-05)


def horner(coefficients, value):
    total = value * coefficients[-1] + coefficients[-2]
    for entry in coefficients[-3::-1]:
        total = total * value + entry
    return total


def green_terms(delta_x, delta_y, delta_z):
    square = delta_x * delta_x + delta_y * delta_y + delta_z * delta_z
    inverse = jnp.where(square < near_limit, 0.0, lax.rsqrt(square))
    radius = square * inverse
    turns = jnp.floor(radius * (0.5 / math.pi) + 0.5)
    angle = (radius * 0.5 - turns * PI_HIGH) - turns * PI_LOW
    angle_sq = angle * angle
    half_sine = angle + angle * (angle_sq * horner(SIN_POLY, angle_sq))
    half_cosine = 1.0 + angle_sq * horner(COS_POLY, angle_sq)
    twice = half_sine + half_sine
    inverse_sq = inverse * inverse
    cube = inverse_sq * inverse
    cosine = (1.0 - twice * half_sine) * cube
    sine = (twice * half_cosine) * cube
    near = square - 1.0
    sine_r = sine * radius
    cosine_r = cosine * radius
    near_re = cosine * near - sine_r
    near_im = sine * near + cosine_r
    mixed_re = cosine + sine_r
    mixed_im = sine - cosine_r
    return (
        near_re,
        near_im,
        (mixed_re + mixed_re - near_re) * inverse_sq,
        (mixed_im + mixed_im - near_im) * inverse_sq,
    )


def split(value):
    high = value.astype(jnp.bfloat16)
    return high, (value - high.astype(jnp.float32)).astype(jnp.bfloat16)


def dot_t(left, right):
    return lax.dot_general(left, right, (((1,), (1,)), ((), ())), preferred_element_type=jnp.float32)


def project_kernel(mode_hbm, moment_hbm, place_hbm, amp_ref, mode_ref, moment_ref, place_ref, mode_sem, sem):
    pieces = PIECES
    depth = mode_ref.shape[0] // pieces
    loads = [
        pltpu.make_async_copy(mode_hbm.at[pl.ds(i * depth, depth)], mode_ref.at[pl.ds(i * depth, depth)], mode_sem.at[i])
        for i in range(pieces)
    ]
    small = [
        pltpu.make_async_copy(moment_hbm, moment_ref, sem.at[0]),
        pltpu.make_async_copy(place_hbm, place_ref, sem.at[1]),
    ]
    small[0].start()
    for load in loads:
        load.start()
    for load in small[1:]:
        load.start()
    small[0].wait()
    plain, swapped = [], []
    for axis_c in range(3):
        plain.append(jnp.concatenate([moment_ref[0, axis_c], moment_ref[1, axis_c]], axis=0))
        swapped.append(
            jnp.concatenate(
                [
                    piece
                    for drive in range(2)
                    for piece in (-moment_ref[drive, axis_c, 1:2, :], moment_ref[drive, axis_c, 0:1, :])
                ],
                axis=0,
            )
        )
    left_high, left_low = split(jnp.concatenate(plain + swapped, axis=1))
    both_left = jnp.concatenate([left_high, left_low], axis=0)
    both, rest = 0.0, 0.0
    for i, load in enumerate(loads):
        load.wait()
        piece = slice(i * depth, (i + 1) * depth)
        mode_high, mode_low = split(mode_ref[piece, :])
        both += jnp.dot(both_left[:, piece], mode_high, preferred_element_type=jnp.float32)
        rest += jnp.dot(left_high[:, piece], mode_low, preferred_element_type=jnp.float32)
    amp = both[0:4] + both[4:8] + rest
    for tile in range(amp.shape[1] // LANES):
        amp_ref[4 * tile : 4 * tile + 4, :] = amp[:, tile * LANES : (tile + 1) * LANES]
    for load in small[1:]:
        load.wait()


def join_kernel(moment_ref, moment_other_ref, place_ref, place_other_ref, amp_ref, out_ref):
    for axis_c in range(3):
        for drive in range(2):
            row = 4 * axis_c + 2 * drive
            out_ref[row : row + 2, :] = jnp.concatenate(
                [moment_ref[drive, axis_c], moment_other_ref[drive, axis_c]], axis=1
            )
    out_ref[12:15, :] = jnp.concatenate([place_ref[...], place_other_ref[...]], axis=1)
    out_ref[15:16, :] = jnp.zeros((1, out_ref.shape[1]), jnp.float32)
    out_ref[ROWS:, :] = amp_ref[...]


def merge_kernel(*refs):
    out_ref = refs[-1]
    rows = refs[0].shape[0] - AMP_ROWS
    for place, ref in enumerate(refs[:-1]):
        out_ref[place * rows : (place + 1) * rows, :] = ref[:rows, :]
    out_ref[(len(refs) - 1) * rows :, :] = sum(ref[rows:, :] for ref in refs[:-1])


def total_kernel(*refs):
    start = refs[0].shape[0] - AMP_ROWS
    refs[-1][...] = sum(ref[start:, :] for ref in refs[:-1])


def prepare_kernel(
    mode_ref, place_ref, moment_ref, detune_hbm, width_hbm, polar_re_hbm, polar_im_hbm,
    high_ref, low_ref, column_ref, centre_ref, straight_ref, crossed_ref, base_ref,
    detune_ref, width_ref, polar_re_ref, polar_im_ref, sem,
):
    loads = [
        pltpu.make_async_copy(source, target, sem.at[i])
        for i, (source, target) in enumerate(
            (
                (detune_hbm, detune_ref),
                (width_hbm, width_ref),
                (polar_re_hbm, polar_re_ref),
                (polar_im_hbm, polar_im_ref),
            )
        )
    ]
    for load in loads:
        load.start()
    high_ref[...], low_ref[...] = split(jnp.transpose(mode_ref[...], (1, 0)))
    targets = place_ref.shape[1]
    for axis_c in range(3):
        row = place_ref[axis_c : axis_c + 1, :]
        column_ref[axis_c] = jnp.transpose(jnp.broadcast_to(row, (LANES, targets)), (1, 0))
        middle = jnp.sum(row, axis=1, keepdims=True) * (1.0 / targets)
        centre_ref[axis_c : axis_c + 1, :] = jnp.broadcast_to(middle, (1, LANES))
    for load in loads:
        load.wait()
    detune, width = detune_ref[...], width_ref[...]
    denominator = detune * detune + width * width
    resp_re, resp_im = detune / denominator, width / denominator
    for tile in range(detune.shape[1] // LANES):
        lanes = slice(tile * LANES, (tile + 1) * LANES)
        for drive in range(2):
            row = 4 * tile + 2 * drive
            straight_ref[row : row + 2, :] = jnp.broadcast_to(resp_re[:, lanes], (2, LANES))
            crossed_ref[row : row + 1, :] = -resp_im[:, lanes]
            crossed_ref[row + 1 : row + 2, :] = resp_im[:, lanes]
    polar_re, polar_im = polar_re_ref[...], polar_im_ref[...]
    for axis_c in range(3):
        for drive in range(2):
            row = 4 * axis_c + 2 * drive
            moment_re = moment_ref[drive, axis_c, 0:1, :]
            moment_im = moment_ref[drive, axis_c, 1:2, :]
            base_ref[row : row + 1, :] = polar_re * moment_re - polar_im * moment_im
            base_ref[row + 1 : row + 2, :] = polar_re * moment_im + polar_im * moment_re


def accumulate_pairs(chips, centre_ref, target_ref, source_refs, before_ref, out_ref, green_ref, feature_ref):
    targets = target_ref.shape[1]
    centre = [centre_ref[axis_c : axis_c + 1, 0:1] for axis_c in range(3)]
    tiles = CHUNK_TILES * len(source_refs)

    def chunk(step, before_ref):
        places = []
        for tile in range(tiles):
            base = (step * CHUNK_TILES + tile % CHUNK_TILES) * ROWS
            if not isinstance(base, int):
                base = pl.multiple_of(base, ROWS)
            block = source_refs[tile // CHUNK_TILES][pl.ds(base, ROWS), :]
            place = [block[12 + axis_c : 13 + axis_c, :] for axis_c in range(3)]
            places.append([jnp.broadcast_to(row, (16, LANES)) for row in place])
            local = [place[axis_c] - centre[axis_c] for axis_c in range(3)]
            moment = [block[4 * axis_c : 4 * axis_c + 4, :] for axis_c in range(3)]
            along = moment[0] * local[0] + moment[1] * local[1] + moment[2] * local[2]
            features = jnp.concatenate(
                [block[:12]]
                + [block[:12] * local[axis_c] for axis_c in range(3)]
                + [along * local[axis_c] for axis_c in range(3)]
                + [jnp.zeros_like(along)],
                axis=0,
            )
            high, (middle, low) = split3(features)
            feature_ref[tile, 0:FEATURES, :] = high
            feature_ref[tile, FEATURES : 2 * FEATURES, :] = middle
            feature_ref[tile, 2 * FEATURES :, :] = low
        for start in range(0, tiles, 2):
            pair_tiles = range(start, start + 2)
            for tile in pair_tiles:
                for group in range(targets // 16):
                    rows = slice(group * 16, group * 16 + 16)
                    deltas = [target_ref[axis_c, rows, :] - places[tile][axis_c] for axis_c in range(3)]
                    for part, entry in enumerate(green_terms(*deltas)):
                        high, rest = split3(entry, part >= 2)
                        for level, value in enumerate((high,) + rest):
                            row = (level * 4 + part - (2 if level == 2 else 0)) * targets + group * 16
                            green_ref[tile, row : row + 16, :] = value

            def green(first, last):
                return jnp.concatenate([green_ref[tile, first * targets : last * targets, :] for tile in pair_tiles], axis=1)

            features = jnp.concatenate([feature_ref[tile] for tile in pair_tiles], axis=1)
            high = dot_t(features, green(0, 4))
            middle = dot_t(features[: 2 * FEATURES], green(4, 8))
            low = dot_t(features[:FEATURES], green(8, 10))
            sums = (high[:FEATURES] + high[FEATURES : 2 * FEATURES] + high[2 * FEATURES :]) + (
                middle[:FEATURES] + middle[FEATURES:]
            )
            half = 2 * targets
            for lanes, extra in ((slice(0, half), 0.0), (slice(half, 2 * half), low)):
                value = sums[:, lanes] + extra
                out_ref[:, lanes] = value if before_ref is None else before_ref[:, lanes] + value
            before_ref = out_ref

    chunk(0, before_ref)
    if chips > CHUNK_TILES:
        pl.loop(1, chips // CHUNK_TILES)(lambda step: chunk(step, out_ref))


def split3(value, three=True):
    high = value.astype(jnp.bfloat16)
    rest = value - high.astype(jnp.float32)
    middle = rest.astype(jnp.bfloat16)
    if not three:
        return high, (middle,)
    return high, (middle, (rest - middle.astype(jnp.float32)).astype(jnp.bfloat16))


def first_pair_kernel(chips, centre_ref, target_ref, source_ref, out_ref, green_ref, feature_ref):
    accumulate_pairs(chips, centre_ref, target_ref, (source_ref,), None, out_ref, green_ref, feature_ref)


def next_pair_kernel(chips, centre_ref, target_ref, source_ref, before_ref, out_ref, green_ref, feature_ref):
    accumulate_pairs(chips, centre_ref, target_ref, (source_ref,), before_ref, out_ref, green_ref, feature_ref)


def complex_rows(real, imag):
    out = []
    for drive in range(2):
        out.append(real[2 * drive : 2 * drive + 1] - imag[2 * drive + 1 : 2 * drive + 2])
        out.append(real[2 * drive + 1 : 2 * drive + 2] + imag[2 * drive : 2 * drive + 1])
    return jnp.concatenate(out, axis=0)


def last_pair_kernel(
    chips, centre_ref, target_ref, side_ref, near_ref, first_ref, place_ref, base_ref, out_ref, sum_ref, green_ref,
    feature_ref,
):
    accumulate_pairs(chips, centre_ref, target_ref, (side_ref, near_ref), first_ref, sum_ref, green_ref, feature_ref)
    targets = place_ref.shape[1]
    raw = sum_ref[...]
    near_re, near_im, far_re, far_im = [raw[:, part * targets : (part + 1) * targets] for part in range(4)]
    local = [place_ref[axis_c : axis_c + 1, :] - centre_ref[axis_c : axis_c + 1, 0:1] for axis_c in range(3)]

    def rows_of(table, group, axis_c):
        return table[12 * group + 4 * axis_c : 12 * group + 4 * axis_c + 4]

    def outer(table, axis_c):
        straight = sum(local[j] * rows_of(table, 0, j) for j in range(3))
        dotted = sum(rows_of(table, 1 + j, j) for j in range(3))
        crossed = sum(local[j] * rows_of(table, 1 + axis_c, j) for j in range(3))
        return local[axis_c] * (straight - dotted) - crossed + rows_of(table, 4, axis_c)

    for axis_c in range(3):
        pair = complex_rows(
            rows_of(near_re, 0, axis_c) + outer(far_re, axis_c), rows_of(near_im, 0, axis_c) + outer(far_im, axis_c)
        )
        out_ref[4 * axis_c : 4 * axis_c + 4, :] = base_ref[4 * axis_c : 4 * axis_c + 4, :] - coupling * pair


def finish_kernel(mine_ref, other_ref, high_ref, low_ref, straight_ref, crossed_ref, rest_ref, out_ref):
    targets = rest_ref.shape[1]
    amp = mine_ref[...] + other_ref[...]
    rows = amp.shape[0]
    odd = (lax.broadcasted_iota(jnp.int32, amp.shape, 0) & 1) == 1
    partner = jnp.where(odd, pltpu.roll(amp, 1, 0), pltpu.roll(amp, rows - 1, 0))
    weighted = straight_ref[...] * amp + crossed_ref[...] * partner
    weighted = jnp.concatenate([weighted[4 * tile : 4 * tile + 4] for tile in range(rows // 4)], axis=1)
    weight_high, weight_low = split(weighted)
    both = jnp.dot(
        jnp.concatenate([weight_high, weight_low], axis=0), high_ref[...], preferred_element_type=jnp.float32
    )
    modal = both[0:4] + both[4:8] + jnp.dot(weight_high, low_ref[...], preferred_element_type=jnp.float32)
    half = 3 * targets
    for axis_c in range(3):
        mode_re = modal[:, axis_c * targets : (axis_c + 1) * targets]
        mode_im = modal[:, half + axis_c * targets : half + (axis_c + 1) * targets]
        result = rest_ref[4 * axis_c : 4 * axis_c + 4, :] - complex_rows(mode_re, mode_im)
        out_ref[0, axis_c] = result[0:2]
        out_ref[1, axis_c] = result[2:4]


def kernel_call(body, outs, operands, scratch=(), flops=100_000, loads=()):
    single = not isinstance(outs, tuple)
    vmem = pl.BlockSpec(memory_space=pltpu.VMEM)
    hbm = pl.BlockSpec(memory_space=pltpu.HBM)
    return pl.pallas_call(
        body,
        out_shape=outs,
        in_specs=[vmem] * len(operands) + [hbm] * len(loads),
        out_specs=vmem if single else (vmem,) * len(outs),
        scratch_shapes=list(scratch),
        cost_estimate=pl.CostEstimate(flops=flops, bytes_accessed=100_000, transcendentals=0),
        compiler_params=pltpu.CompilerParams(vmem_limit_bytes=12 * 1024 * 1024),
    )(*operands, *loads)


def on_device(devices, positions, moments, inv_polar_re, inv_polar_im, mode_field, mode_detune, mode_width):
    targets = positions.shape[1]
    modes = mode_field.shape[3]

    def shape(*dims, dtype=jnp.float32):
        return jax.ShapeDtypeStruct(dims, dtype)

    def exchange(value, distance):
        return lax.ppermute(value, AXES, [(i, i ^ distance) for i in range(devices)])

    def like(value):
        return shape(*value.shape)

    moments = jnp.transpose(moments, (0, 2, 1, 3))
    mode_rows = mode_field.reshape(6 * targets, modes)
    moments_other = exchange(moments, 1)
    positions_other = exchange(positions, 1)

    def in_hbm(*values):
        return tuple(pltpu.with_memory_space_constraint(value, pltpu.HBM) for value in values)

    inputs = in_hbm(mode_rows, moments, positions)
    amp, mode_rows, moments, positions = kernel_call(
        project_kernel,
        (shape(AMP_ROWS, LANES),) + tuple(like(value) for value in inputs),
        (),
        [pltpu.SemaphoreType.DMA((PIECES,)), pltpu.SemaphoreType.DMA((2,))],
        flops=5_000_000,
        loads=inputs,
    )
    message = kernel_call(
        join_kernel, shape(ROWS + AMP_ROWS, LANES), (moments, moments_other, positions, positions_other, amp)
    )
    mode_high, mode_low, columns, centre, straight, crossed, base = kernel_call(
        prepare_kernel,
        (
            shape(modes, 6 * targets, dtype=jnp.bfloat16),
            shape(modes, 6 * targets, dtype=jnp.bfloat16),
            shape(3, targets, LANES),
            shape(8, LANES),
            shape(AMP_ROWS, LANES),
            shape(AMP_ROWS, LANES),
            shape(12, targets),
        ),
        (mode_rows, positions, moments),
        [
            pltpu.VMEM((1, modes), jnp.float32),
            pltpu.VMEM((1, modes), jnp.float32),
            pltpu.VMEM((1, targets), jnp.float32),
            pltpu.VMEM((1, targets), jnp.float32),
            pltpu.SemaphoreType.DMA((4,)),
        ],
        flops=5_000_000,
        loads=in_hbm(mode_detune[None], mode_width[None], inv_polar_re[None], inv_polar_im[None]),
    )
    distance = devices // 2
    while distance > 4:
        steps = ((3 * distance // 2) ^ 1, distance ^ 1, distance // 2) if distance > 8 else (distance ^ 1,)
        arrived = [exchange(message, step) for step in steps]
        rows = message.shape[0] - AMP_ROWS
        message = kernel_call(merge_kernel, shape((1 + len(steps)) * rows + AMP_ROWS, LANES), (message, *arrived))
        distance //= 4 if len(steps) == 3 else 2
    chips = (message.shape[0] - AMP_ROWS) // ROWS
    diagonal = exchange(message, 6)
    side = exchange(message, 4 ^ 1)
    near = exchange(message, 2 ^ 1)
    sums = shape(FEATURES, 4 * targets)

    def pair(kernel, sources, *more, out=sums, extra=()):
        tiles = CHUNK_TILES * len(sources)
        return kernel_call(
            functools.partial(kernel, chips),
            out,
            (centre, columns) + sources + more,
            list(extra)
            + [
                pltpu.VMEM((tiles, 10 * targets, LANES), jnp.bfloat16),
                pltpu.VMEM((tiles, 3 * FEATURES, LANES), jnp.bfloat16),
            ],
            flops=20_000_000,
        )

    partial_sums = pair(first_pair_kernel, (message,))
    partial_sums = pair(next_pair_kernel, (diagonal,), partial_sums)
    mine = kernel_call(total_kernel, shape(AMP_ROWS, LANES), (message, diagonal, side, near))
    other = exchange(mine, 1)
    rest = pair(
        last_pair_kernel,
        (side, near),
        partial_sums,
        positions,
        base,
        out=shape(12, targets),
        extra=(pltpu.VMEM(sums.shape, jnp.float32),),
    )
    out = kernel_call(
        finish_kernel, shape(2, 3, 2, targets), (mine, other, mode_high, mode_low, straight, crossed, rest)
    )
    return jnp.transpose(out, (0, 2, 1, 3))


def solution(mesh):
    placed = (
        P(None, AXES),
        P(None, None, None, AXES),
        P(AXES),
        P(AXES),
        P(None, None, AXES, None),
        P(),
        P(),
    )
    return jax.shard_map(
        functools.partial(on_device, mesh.size),
        mesh=mesh,
        in_specs=placed,
        out_specs=P(None, None, None, AXES),
        check_vma=False,
    )
```

```python
import functools
import math

import jax
import jax.numpy as jnp
from jax import lax
from jax.experimental import pallas as pl
from jax.experimental.pallas import tpu as pltpu
from jax.sharding import PartitionSpec as P


coupling = 0.05
near_limit = 0.04

AXES = ("blk", "grp")
LANES = 128
ROWS = 16
CHUNK_TILES = 4
PIECES = 3
AMP_ROWS = 16
FEATURES = 64

PI_HIGH = 3.140625
PI_LOW = math.pi - PI_HIGH
SIN_POLY = (-0.16666656732559204, 0.008332998491823673, -0.00019805235206149518, 2.5970118713303236e-06)
COS_POLY = (-0.4999992549419403, 0.04166382923722267, -0.0013854617718607187, 2.316308928129729e-05)


def horner(coefficients, value):
    total = value * coefficients[-1] + coefficients[-2]
    for entry in coefficients[-3::-1]:
        total = total * value + entry
    return total


def green_terms(delta_x, delta_y, delta_z):
    square = delta_x * delta_x + delta_y * delta_y + delta_z * delta_z
    inverse = jnp.where(square < near_limit, 0.0, lax.rsqrt(square))
    radius = square * inverse
    turns = jnp.floor(radius * (0.5 / math.pi) + 0.5)
    angle = (radius * 0.5 - turns * PI_HIGH) - turns * PI_LOW
    angle_sq = angle * angle
    half_sine = angle + angle * (angle_sq * horner(SIN_POLY, angle_sq))
    half_cosine = 1.0 + angle_sq * horner(COS_POLY, angle_sq)
    twice = half_sine + half_sine
    inverse_sq = inverse * inverse
    cube = inverse_sq * inverse
    cosine = (1.0 - twice * half_sine) * cube
    sine = (twice * half_cosine) * cube
    near = square - 1.0
    sine_r = sine * radius
    cosine_r = cosine * radius
    near_re = cosine * near - sine_r
    near_im = sine * near + cosine_r
    mixed_re = cosine + sine_r
    mixed_im = sine - cosine_r
    return (
        near_re,
        near_im,
        (mixed_re + mixed_re - near_re) * inverse_sq,
        (mixed_im + mixed_im - near_im) * inverse_sq,
    )


def split(value):
    high = value.astype(jnp.bfloat16)
    return high, (value - high.astype(jnp.float32)).astype(jnp.bfloat16)


def dot_t(left, right):
    return lax.dot_general(left, right, (((1,), (1,)), ((), ())), preferred_element_type=jnp.float32)


def project_kernel(mode_hbm, moment_hbm, place_hbm, amp_ref, mode_ref, moment_ref, place_ref, mode_sem, sem):
    pieces = PIECES
    depth = mode_ref.shape[0] // pieces
    loads = [
        pltpu.make_async_copy(mode_hbm.at[pl.ds(i * depth, depth)], mode_ref.at[pl.ds(i * depth, depth)], mode_sem.at[i])
        for i in range(pieces)
    ]
    small = [
        pltpu.make_async_copy(moment_hbm, moment_ref, sem.at[0]),
        pltpu.make_async_copy(place_hbm, place_ref, sem.at[1]),
    ]
    small[0].start()
    for load in loads:
        load.start()
    for load in small[1:]:
        load.start()
    small[0].wait()
    plain, swapped = [], []
    for axis_c in range(3):
        plain.append(jnp.concatenate([moment_ref[0, axis_c], moment_ref[1, axis_c]], axis=0))
        swapped.append(
            jnp.concatenate(
                [
                    piece
                    for drive in range(2)
                    for piece in (-moment_ref[drive, axis_c, 1:2, :], moment_ref[drive, axis_c, 0:1, :])
                ],
                axis=0,
            )
        )
    left_high, left_low = split(jnp.concatenate(plain + swapped, axis=1))
    both_left = jnp.concatenate([left_high, left_low], axis=0)
    both, rest = 0.0, 0.0
    for i, load in enumerate(loads):
        load.wait()
        piece = slice(i * depth, (i + 1) * depth)
        mode_high, mode_low = split(mode_ref[piece, :])
        both += jnp.dot(both_left[:, piece], mode_high, preferred_element_type=jnp.float32)
        rest += jnp.dot(left_high[:, piece], mode_low, preferred_element_type=jnp.float32)
    amp = both[0:4] + both[4:8] + rest
    for tile in range(amp.shape[1] // LANES):
        amp_ref[4 * tile : 4 * tile + 4, :] = amp[:, tile * LANES : (tile + 1) * LANES]
    for load in small[1:]:
        load.wait()


def join_kernel(moment_ref, moment_other_ref, place_ref, place_other_ref, amp_ref, out_ref):
    for axis_c in range(3):
        for drive in range(2):
            row = 4 * axis_c + 2 * drive
            out_ref[row : row + 2, :] = jnp.concatenate(
                [moment_ref[drive, axis_c], moment_other_ref[drive, axis_c]], axis=1
            )
    out_ref[12:15, :] = jnp.concatenate([place_ref[...], place_other_ref[...]], axis=1)
    out_ref[15:16, :] = jnp.zeros((1, out_ref.shape[1]), jnp.float32)
    out_ref[ROWS:, :] = amp_ref[...]


def merge_kernel(*refs):
    out_ref = refs[-1]
    rows = refs[0].shape[0] - AMP_ROWS
    for place, ref in enumerate(refs[:-1]):
        out_ref[place * rows : (place + 1) * rows, :] = ref[:rows, :]
    out_ref[(len(refs) - 1) * rows :, :] = sum(ref[rows:, :] for ref in refs[:-1])


def total_kernel(*refs):
    start = refs[0].shape[0] - AMP_ROWS
    refs[-1][...] = sum(ref[start:, :] for ref in refs[:-1])


def prepare_kernel(
    mode_ref, place_ref, moment_ref, detune_hbm, width_hbm, polar_re_hbm, polar_im_hbm,
    high_ref, low_ref, column_ref, centre_ref, straight_ref, crossed_ref, base_ref,
    detune_ref, width_ref, polar_re_ref, polar_im_ref, sem,
):
    loads = [
        pltpu.make_async_copy(source, target, sem.at[i])
        for i, (source, target) in enumerate(
            (
                (detune_hbm, detune_ref),
                (width_hbm, width_ref),
                (polar_re_hbm, polar_re_ref),
                (polar_im_hbm, polar_im_ref),
            )
        )
    ]
    for load in loads:
        load.start()
    high_ref[...], low_ref[...] = split(jnp.transpose(mode_ref[...], (1, 0)))
    targets = place_ref.shape[1]
    for axis_c in range(3):
        row = place_ref[axis_c : axis_c + 1, :]
        column_ref[axis_c] = jnp.transpose(jnp.broadcast_to(row, (LANES, targets)), (1, 0))
        middle = jnp.sum(row, axis=1, keepdims=True) * (1.0 / targets)
        centre_ref[axis_c : axis_c + 1, :] = jnp.broadcast_to(middle, (1, LANES))
    for load in loads:
        load.wait()
    detune, width = detune_ref[...], width_ref[...]
    denominator = detune * detune + width * width
    resp_re, resp_im = detune / denominator, width / denominator
    for tile in range(detune.shape[1] // LANES):
        lanes = slice(tile * LANES, (tile + 1) * LANES)
        for drive in range(2):
            row = 4 * tile + 2 * drive
            straight_ref[row : row + 2, :] = jnp.broadcast_to(resp_re[:, lanes], (2, LANES))
            crossed_ref[row : row + 1, :] = -resp_im[:, lanes]
            crossed_ref[row + 1 : row + 2, :] = resp_im[:, lanes]
    polar_re, polar_im = polar_re_ref[...], polar_im_ref[...]
    for axis_c in range(3):
        for drive in range(2):
            row = 4 * axis_c + 2 * drive
            moment_re = moment_ref[drive, axis_c, 0:1, :]
            moment_im = moment_ref[drive, axis_c, 1:2, :]
            base_ref[row : row + 1, :] = polar_re * moment_re - polar_im * moment_im
            base_ref[row + 1 : row + 2, :] = polar_re * moment_im + polar_im * moment_re


def accumulate_pairs(chips, centre_ref, target_ref, source_refs, before_ref, out_ref, green_ref, feature_ref):
    targets = target_ref.shape[1]
    centre = [centre_ref[axis_c : axis_c + 1, 0:1] for axis_c in range(3)]
    tiles = CHUNK_TILES * len(source_refs)

    def chunk(step, before_ref):
        for start in range(0, tiles, 2):
            pair_tiles = range(start, start + 2)
            places = {}
            for tile in pair_tiles:
                base = (step * CHUNK_TILES + tile % CHUNK_TILES) * ROWS
                if not isinstance(base, int):
                    base = pl.multiple_of(base, ROWS)
                block = source_refs[tile // CHUNK_TILES][pl.ds(base, ROWS), :]
                place = [block[12 + axis_c : 13 + axis_c, :] for axis_c in range(3)]
                places[tile] = [jnp.broadcast_to(row, (16, LANES)) for row in place]
                local = [place[axis_c] - centre[axis_c] for axis_c in range(3)]
                moment = [block[4 * axis_c : 4 * axis_c + 4, :] for axis_c in range(3)]
                along = moment[0] * local[0] + moment[1] * local[1] + moment[2] * local[2]
                features = jnp.concatenate(
                    [block[:12]]
                    + [block[:12] * local[axis_c] for axis_c in range(3)]
                    + [along * local[axis_c] for axis_c in range(3)]
                    + [jnp.zeros_like(along)],
                    axis=0,
                )
                high, (middle, low) = split3(features)
                feature_ref[tile, 0:FEATURES, :] = high
                feature_ref[tile, FEATURES : 2 * FEATURES, :] = middle
                feature_ref[tile, 2 * FEATURES :, :] = low
            for tile in pair_tiles:
                for group in range(targets // 16):
                    rows = slice(group * 16, group * 16 + 16)
                    deltas = [target_ref[axis_c, rows, :] - places[tile][axis_c] for axis_c in range(3)]
                    for part, entry in enumerate(green_terms(*deltas)):
                        high, rest = split3(entry, part >= 2)
                        for level, value in enumerate((high,) + rest):
                            row = (level * 4 + part - (2 if level == 2 else 0)) * targets + group * 16
                            green_ref[tile, row : row + 16, :] = value

            def green(first, last):
                return jnp.concatenate([green_ref[tile, first * targets : last * targets, :] for tile in pair_tiles], axis=1)

            features = jnp.concatenate([feature_ref[tile] for tile in pair_tiles], axis=1)
            high = dot_t(features, green(0, 4))
            middle = dot_t(features[: 2 * FEATURES], green(4, 8))
            low = dot_t(features[:FEATURES], green(8, 10))
            sums = (high[:FEATURES] + high[FEATURES : 2 * FEATURES] + high[2 * FEATURES :]) + (
                middle[:FEATURES] + middle[FEATURES:]
            )
            half = 2 * targets
            for lanes, extra in ((slice(0, half), 0.0), (slice(half, 2 * half), low)):
                value = sums[:, lanes] + extra
                out_ref[:, lanes] = value if before_ref is None else before_ref[:, lanes] + value
            before_ref = out_ref

    chunk(0, before_ref)
    if chips > CHUNK_TILES:
        pl.loop(1, chips // CHUNK_TILES)(lambda step: chunk(step, out_ref))


def split3(value, three=True):
    high = value.astype(jnp.bfloat16)
    rest = value - high.astype(jnp.float32)
    middle = rest.astype(jnp.bfloat16)
    if not three:
        return high, (middle,)
    return high, (middle, (rest - middle.astype(jnp.float32)).astype(jnp.bfloat16))


def first_pair_kernel(chips, centre_ref, target_ref, source_ref, out_ref, green_ref, feature_ref):
    accumulate_pairs(chips, centre_ref, target_ref, (source_ref,), None, out_ref, green_ref, feature_ref)


def next_pair_kernel(chips, centre_ref, target_ref, source_ref, before_ref, out_ref, green_ref, feature_ref):
    accumulate_pairs(chips, centre_ref, target_ref, (source_ref,), before_ref, out_ref, green_ref, feature_ref)


def complex_rows(real, imag):
    out = []
    for drive in range(2):
        out.append(real[2 * drive : 2 * drive + 1] - imag[2 * drive + 1 : 2 * drive + 2])
        out.append(real[2 * drive + 1 : 2 * drive + 2] + imag[2 * drive : 2 * drive + 1])
    return jnp.concatenate(out, axis=0)


def last_pair_kernel(
    chips, centre_ref, target_ref, side_ref, near_ref, first_ref, place_ref, base_ref, out_ref, sum_ref, green_ref,
    feature_ref,
):
    accumulate_pairs(chips, centre_ref, target_ref, (side_ref, near_ref), first_ref, sum_ref, green_ref, feature_ref)
    targets = place_ref.shape[1]
    raw = sum_ref[...]
    near_re, near_im, far_re, far_im = [raw[:, part * targets : (part + 1) * targets] for part in range(4)]
    local = [place_ref[axis_c : axis_c + 1, :] - centre_ref[axis_c : axis_c + 1, 0:1] for axis_c in range(3)]

    def rows_of(table, group, axis_c):
        return table[12 * group + 4 * axis_c : 12 * group + 4 * axis_c + 4]

    def outer(table, axis_c):
        straight = sum(local[j] * rows_of(table, 0, j) for j in range(3))
        dotted = sum(rows_of(table, 1 + j, j) for j in range(3))
        crossed = sum(local[j] * rows_of(table, 1 + axis_c, j) for j in range(3))
        return local[axis_c] * (straight - dotted) - crossed + rows_of(table, 4, axis_c)

    for axis_c in range(3):
        pair = complex_rows(
            rows_of(near_re, 0, axis_c) + outer(far_re, axis_c), rows_of(near_im, 0, axis_c) + outer(far_im, axis_c)
        )
        out_ref[4 * axis_c : 4 * axis_c + 4, :] = base_ref[4 * axis_c : 4 * axis_c + 4, :] - coupling * pair


def finish_kernel(mine_ref, other_ref, high_ref, low_ref, straight_ref, crossed_ref, rest_ref, out_ref):
    targets = rest_ref.shape[1]
    amp = mine_ref[...] + other_ref[...]
    rows = amp.shape[0]
    odd = (lax.broadcasted_iota(jnp.int32, amp.shape, 0) & 1) == 1
    partner = jnp.where(odd, pltpu.roll(amp, 1, 0), pltpu.roll(amp, rows - 1, 0))
    weighted = straight_ref[...] * amp + crossed_ref[...] * partner
    weighted = jnp.concatenate([weighted[4 * tile : 4 * tile + 4] for tile in range(rows // 4)], axis=1)
    weight_high, weight_low = split(weighted)
    both = jnp.dot(
        jnp.concatenate([weight_high, weight_low], axis=0), high_ref[...], preferred_element_type=jnp.float32
    )
    modal = both[0:4] + both[4:8] + jnp.dot(weight_high, low_ref[...], preferred_element_type=jnp.float32)
    half = 3 * targets
    for axis_c in range(3):
        mode_re = modal[:, axis_c * targets : (axis_c + 1) * targets]
        mode_im = modal[:, half + axis_c * targets : half + (axis_c + 1) * targets]
        result = rest_ref[4 * axis_c : 4 * axis_c + 4, :] - complex_rows(mode_re, mode_im)
        out_ref[0, axis_c] = result[0:2]
        out_ref[1, axis_c] = result[2:4]


def kernel_call(body, outs, operands, scratch=(), flops=100_000, loads=()):
    single = not isinstance(outs, tuple)
    vmem = pl.BlockSpec(memory_space=pltpu.VMEM)
    hbm = pl.BlockSpec(memory_space=pltpu.HBM)
    return pl.pallas_call(
        body,
        out_shape=outs,
        in_specs=[vmem] * len(operands) + [hbm] * len(loads),
        out_specs=vmem if single else (vmem,) * len(outs),
        scratch_shapes=list(scratch),
        cost_estimate=pl.CostEstimate(flops=flops, bytes_accessed=100_000, transcendentals=0),
        compiler_params=pltpu.CompilerParams(vmem_limit_bytes=12 * 1024 * 1024),
    )(*operands, *loads)


def on_device(devices, positions, moments, inv_polar_re, inv_polar_im, mode_field, mode_detune, mode_width):
    targets = positions.shape[1]
    modes = mode_field.shape[3]

    def shape(*dims, dtype=jnp.float32):
        return jax.ShapeDtypeStruct(dims, dtype)

    def exchange(value, distance):
        return lax.ppermute(value, AXES, [(i, i ^ distance) for i in range(devices)])

    def like(value):
        return shape(*value.shape)

    moments = jnp.transpose(moments, (0, 2, 1, 3))
    mode_rows = mode_field.reshape(6 * targets, modes)
    moments_other = exchange(moments, 1)
    positions_other = exchange(positions, 1)

    def in_hbm(*values):
        return tuple(pltpu.with_memory_space_constraint(value, pltpu.HBM) for value in values)

    inputs = in_hbm(mode_rows, moments, positions)
    amp, mode_rows, moments, positions = kernel_call(
        project_kernel,
        (shape(AMP_ROWS, LANES),) + tuple(like(value) for value in inputs),
        (),
        [pltpu.SemaphoreType.DMA((PIECES,)), pltpu.SemaphoreType.DMA((2,))],
        flops=5_000_000,
        loads=inputs,
    )
    message = kernel_call(
        join_kernel, shape(ROWS + AMP_ROWS, LANES), (moments, moments_other, positions, positions_other, amp)
    )
    mode_high, mode_low, columns, centre, straight, crossed, base = kernel_call(
        prepare_kernel,
        (
            shape(modes, 6 * targets, dtype=jnp.bfloat16),
            shape(modes, 6 * targets, dtype=jnp.bfloat16),
            shape(3, targets, LANES),
            shape(8, LANES),
            shape(AMP_ROWS, LANES),
            shape(AMP_ROWS, LANES),
            shape(12, targets),
        ),
        (mode_rows, positions, moments),
        [
            pltpu.VMEM((1, modes), jnp.float32),
            pltpu.VMEM((1, modes), jnp.float32),
            pltpu.VMEM((1, targets), jnp.float32),
            pltpu.VMEM((1, targets), jnp.float32),
            pltpu.SemaphoreType.DMA((4,)),
        ],
        flops=5_000_000,
        loads=in_hbm(mode_detune[None], mode_width[None], inv_polar_re[None], inv_polar_im[None]),
    )
    distance = devices // 2
    while distance > 4:
        steps = ((3 * distance // 2) ^ 1, distance ^ 1, distance // 2) if distance > 8 else (distance ^ 1,)
        arrived = [exchange(message, step) for step in steps]
        rows = message.shape[0] - AMP_ROWS
        message = kernel_call(merge_kernel, shape((1 + len(steps)) * rows + AMP_ROWS, LANES), (message, *arrived))
        distance //= 4 if len(steps) == 3 else 2
    chips = (message.shape[0] - AMP_ROWS) // ROWS
    diagonal = exchange(message, 6)
    side = exchange(message, 4 ^ 1)
    near = exchange(message, 2 ^ 1)
    sums = shape(FEATURES, 4 * targets)

    def pair(kernel, sources, *more, out=sums, extra=()):
        tiles = CHUNK_TILES * len(sources)
        return kernel_call(
            functools.partial(kernel, chips),
            out,
            (centre, columns) + sources + more,
            list(extra)
            + [
                pltpu.VMEM((tiles, 10 * targets, LANES), jnp.bfloat16),
                pltpu.VMEM((tiles, 3 * FEATURES, LANES), jnp.bfloat16),
            ],
            flops=20_000_000,
        )

    partial_sums = pair(first_pair_kernel, (message,))
    partial_sums = pair(next_pair_kernel, (diagonal,), partial_sums)
    mine = kernel_call(total_kernel, shape(AMP_ROWS, LANES), (message, diagonal, side, near))
    other = exchange(mine, 1)
    rest = pair(
        last_pair_kernel,
        (side, near),
        partial_sums,
        positions,
        base,
        out=shape(12, targets),
        extra=(pltpu.VMEM(sums.shape, jnp.float32),),
    )
    out = kernel_call(
        finish_kernel, shape(2, 3, 2, targets), (mine, other, mode_high, mode_low, straight, crossed, rest)
    )
    return jnp.transpose(out, (0, 2, 1, 3))


def solution(mesh):
    placed = (
        P(None, AXES),
        P(None, None, None, AXES),
        P(AXES),
        P(AXES),
        P(None, None, AXES, None),
        P(),
        P(),
    )
    return jax.shard_map(
        functools.partial(on_device, mesh.size),
        mesh=mesh,
        in_specs=placed,
        out_specs=P(None, None, None, AXES),
        check_vma=False,
    )
```
